128 devices in a mesh: gx: 4 (over z), gy: 16 (over y, x), gz: 2 (over core).
Axes of the slice: x: 4, y: 4, z: 4, core: 2. Of those that a mesh axis runs over, the one named last changes fastest.
Arguments:
- particles: float32 [8, 1048576], P(None, ('gx', 'gy', 'gz')), may hold values from -0.5 to 0.5
- dest_key: int32 [1048576], P(('gx', 'gy', 'gz')), may hold values from 0 to 127, as said below
- cell_a: int32 [1048576], P(('gx', 'gy', 'gz')), may hold values from 0 to 255
- cell_b: int32 [1048576], P(('gx', 'gy', 'gz')), may hold values from 0 to 127
- velocity: float32 [2, 1024, 4096], P(None, 'gx', ('gy', 'gz')), may hold values from -6 to 6
Outputs:
- binned: float32 [8, 4194304], P(None, ('gx', 'gy', 'gz'))
- binned_cell: int32 [4194304], P(('gx', 'gy', 'gz'))
The draws below stay inside these ranges and needn't reach their ends.
Inputs may be any that keep to these rules, and one draw needn't show every extreme that they name: Of the particles of one device at most 256 have any one value of dest_key, and one device is named by exactly 256 particles of every device.
All inputs are finite; a program needn't handle non-finite values.
Results may differ from the reference program's by a relative error of at most 0.0003.
Values sent between devices are 32-bit elements; how exact they have to be, the bound alone decides.
A program may use at most 64 MiB of HBM per device.

```python
import jax
import jax.numpy as jnp
from jax import lax

P_DEV = 8192
TA = 256
TB = 128
OWNERS = 128
CAP = 256
TOTAL = 1048576
NA = 1024
NB = 4096
N_GY = 16
N_GZ = 2


def draw_dest_key(key, part):
    hot_owner = jax.random.randint(jax.random.fold_in(key, 7), (), 0, OWNERS)
    slot_owner = (jnp.arange(OWNERS * CAP, dtype=jnp.int32) // CAP + hot_owner) % OWNERS

    def one_source(source_dev):
        source_key = jax.random.fold_in(key, source_dev)
        others = jax.random.permutation(source_key, OWNERS * CAP - CAP).astype(jnp.int32) + CAP
        chosen = jnp.concatenate([jnp.arange(CAP, dtype=jnp.int32), others[:P_DEV - CAP]])
        shuffle = jax.random.permutation(jax.random.fold_in(source_key, 1), P_DEV)
        return slot_owner[chosen][shuffle]
    return lax.map(one_source, jnp.arange(OWNERS, dtype=jnp.int32)).reshape(-1)


def place_ends(array, stream_key, smallest, top_value):
    longest = array.shape.index(max(array.shape))
    spots = []
    for shift in (0, 1):
        where = [jax.random.randint(jax.random.fold_in(stream_key, axis), (), 0, length) for axis, length in enumerate(array.shape)]
        where[longest] = (where[longest] + shift) % array.shape[longest]
        spots.append(tuple(where))
    return array.at[spots[0]].set(smallest).at[spots[1]].set(top_value)


def level_of(rng, extent, split, low, high):
    def one(dim, shards_of):
        heights = jax.random.uniform(jax.random.fold_in(jax.random.fold_in(rng, 6), dim), (shards_of,), jnp.float32, low / len(split), high / len(split))
        return jnp.repeat(jnp.exp(heights), extent[dim] // shards_of).reshape((-1,) + (1,) * (len(extent) - dim - 1))

    gain = one(*split[0])
    for cut in split[1:]:
        gain = gain * one(*cut)
    return gain


def scatter_about(key, shape, spread, limit, cuts=(), held_as=jnp.bfloat16):
    drawn = spread * jax.random.normal(key, shape, jnp.float32)
    if cuts:
        drawn = drawn * level_of(key, shape, cuts, -0.22, 0.18)
    return jnp.clip(drawn, -limit, limit).astype(held_as)


def setup_inputs(seed: int = 0) -> dict:
    splits = jax.random.split(jax.random.key(seed), 6)
    particles = jnp.clip(jax.random.uniform(splits[0], (8, TOTAL), jnp.float32, -0.5, 0.5) * level_of(splits[0], (8, TOTAL), ((1, 128),), -0.4, 0.0), -0.5, 0.5)
    dest_key = draw_dest_key(jax.random.fold_in(splits[5], 71), 0)
    cell_a = place_ends(jax.random.randint(splits[2], (TOTAL,), 0, TA), jax.random.fold_in(splits[2], 1), 0, TA - 1).astype(jnp.int32)
    cell_b = place_ends(jax.random.randint(splits[3], (TOTAL,), 0, TB), jax.random.fold_in(splits[3], 1), 0, TB - 1).astype(jnp.int32)
    velocity = scatter_about(splits[4], (2, NA, NB), 1.0, 6.0, ((1, 4), (2, 32)), jnp.float32)
    return {"particles": particles, "dest_key": dest_key, "cell_a": cell_a, "cell_b": cell_b, "velocity": velocity}


step_length = 0.5


def quad_weights(frac):
    return (0.5 * frac * (frac - 1.0), 1.0 - frac * frac, 0.5 * frac * (frac + 1.0))


def reference(particles, dest_key, cell_a, cell_b, velocity):
    source_dev = jnp.arange(TOTAL, dtype=jnp.int32) // P_DEV
    bucket_key = source_dev * OWNERS + dest_key
    ordering = jnp.argsort(bucket_key, stable=True).astype(jnp.int32)
    ordered = bucket_key[ordering]
    first_index = jnp.searchsorted(ordered, ordered, side="left").astype(jnp.int32)
    rank_sorted = jnp.arange(TOTAL, dtype=jnp.int32) - first_index
    ranking = jnp.zeros((TOTAL,), jnp.int32).at[ordering].set(rank_sorted)
    slot_index = dest_key * (OWNERS * CAP) + source_dev * CAP + ranking
    tile_columns = N_GY * N_GZ
    global_a = (dest_key // tile_columns) * TA + cell_a
    global_b = (dest_key % tile_columns) * TB + cell_b
    padded = jnp.pad(velocity, ((0, 0), (1, 1), (1, 1)))
    row_stride = NB + 2
    flat_field = padded.reshape(2, -1)
    center = ((global_a + 1) * row_stride + global_b + 1).astype(jnp.int32)
    weights_a = quad_weights(particles[0])
    weights_b = quad_weights(particles[1])
    speed = jnp.zeros((2, TOTAL), jnp.float32)
    for shift_a in range(3):
        for shift_b in range(3):
            nodes = flat_field[:, center + (shift_a - 1) * row_stride + (shift_b - 1)]
            speed = speed + weights_a[shift_a] * weights_b[shift_b] * nodes
    advanced = jnp.concatenate([particles[0:2], particles[2:4] + step_length * speed, particles[4:8]], axis=0)
    binned = jnp.zeros((8, OWNERS * OWNERS * CAP), particles.dtype).at[:, slot_index].set(advanced)
    binned_cell = jnp.full((OWNERS * OWNERS * CAP,), -1, jnp.int32).at[slot_index].set(cell_a * TB + cell_b)
    return binned, binned_cell
```

```python
import jax
import jax.numpy as jnp
from jax import lax
from jax.experimental import pallas as pl
from jax.experimental.pallas import tpu as pltpu
from jax.sharding import PartitionSpec as P

BF = jnp.bfloat16
F32 = jnp.float32
I32 = jnp.int32
NT = (((1,), (1,)), ((), ()))
AXES = ("gx", "gy", "gz")
MESH = pl.DeviceIdType.MESH


def dotf(a, b):
    return jnp.dot(a, b, preferred_element_type=F32)


def row256(ref, j):
    r = ref[pl.ds(2*j,2),:]
    return jnp.concatenate([r[0:1],r[1:2]],axis=1)

def bucket(part, dest, ca, cb, out, cells, oh, srt, csrt, acc, stv, sts, sem):
    nb=32
    iod=lax.broadcasted_iota(I32,(128,256),0).astype(F32).astype(BF)
    one=jnp.ones((),BF); zero=jnp.zeros((),BF)
    def onehot(j,S):
        d=row256(dest,j).astype(F32).astype(BF)
        o=jnp.where(iod==jnp.broadcast_to(d,(128,256)),one,zero)
        oh[j]=o
        return S+o
    S=lax.fori_loop(0,nb,onehot,jnp.zeros((128,256),BF),unroll=4)
    ones=jnp.ones((256,256),BF)
    tot=dotf(S,ones)
    low=(lax.broadcasted_iota(I32,(128,128),0)>lax.broadcasted_iota(I32,(128,128),1)).astype(F32).astype(BF)
    start=dotf(low,tot.astype(BF))
    diag=lax.broadcasted_iota(I32,(128,128),0)==lax.broadcasted_iota(I32,(128,128),1)
    srow=jnp.sum(jnp.where(diag,start[:,:128],0.),axis=0,keepdims=True)
    trow=jnp.sum(jnp.where(diag,tot[:,:128],0.),axis=0,keepdims=True)
    stv[0:1,:]=srow.astype(I32)
    stv[1:2,:]=trow.astype(I32)
    cp=pltpu.make_async_copy(stv,sts,sem)
    cp.start()
    up=(lax.broadcasted_iota(I32,(256,256),0)<lax.broadcasted_iota(I32,(256,256),1)).astype(F32).astype(BF)
    acc[...]=jnp.zeros_like(acc)
    iol=lax.broadcasted_iota(I32,(256,256),0).astype(F32).astype(BF)
    hrow=(lax.broadcasted_iota(I32,(256,256),0)//8).astype(F32).astype(BF)
    hrow32=lax.broadcasted_iota(I32,(32,256),0).astype(F32).astype(BF)
    UB=2
    def place(jj,base):
        tot=None
        for u in range(UB):
            j=jj*UB+u
            o=oh[j]
            before=dotf(o,up)
            cnt=dotf(o,ones)
            pos=jnp.sum(o.astype(F32)*(before+base),axis=0,keepdims=True)
            base=base+cnt
            hi=jnp.floor(pos*(1/256)); lo=pos-256*hi
            hib=jnp.broadcast_to(hi.astype(BF),(256,256)); lob=jnp.broadcast_to(lo.astype(BF),(256,256))
            lot=jnp.where(iol==lob,one,zero)
            v=part[:,pl.ds(pl.multiple_of(j*256,256),256)]
            vh=v.astype(BF); vl=(v-vh.astype(F32)).astype(BF)
            m=hrow==hib
            vh2=jnp.concatenate([vh]*32,axis=0)
            vl2=jnp.concatenate([vl]*32,axis=0)
            m32=hrow32==hib[:32]
            a=row256(ca,j).astype(F32).astype(BF); b=row256(cb,j).astype(F32).astype(BF)
            A=jnp.concatenate([jnp.where(m,vh2,zero),jnp.where(m,vl2,zero),
               jnp.where(m32,jnp.broadcast_to(a,(32,256)),zero),jnp.where(m32,jnp.broadcast_to(b,(32,256)),zero)],axis=0)
            x=lax.dot_general(A,lot,NT,preferred_element_type=F32)
            tot = x if tot is None else tot+x
        acc[...]+=tot
        return base
    lax.fori_loop(0,nb//UB,place,start)
    for h in range(32):
        srt[:,h*256:(h+1)*256]=acc[h*8:(h+1)*8]+acc[256+h*8:256+(h+1)*8]
    cc=acc[512:544]*128.+acc[544:576]
    for h in range(32):
        csrt[0:1,h*256:(h+1)*256]=cc[h:h+1]
    cp.wait()
    lane=lax.broadcasted_iota(I32,(8,128),1)
    lane1=lane[0:1]
    def expand(d,_):
        s=sts[0,d]; n=sts[1,d]
        al=pl.multiple_of((s//128)*128,128); sh=s%128
        rot=(128-sh)%128
        x=srt[:,pl.ds(al,384)]
        c=csrt[:,pl.ds(al,384)]
        rs=[pltpu.roll(x[:,128*i:128*(i+1)],rot,1) for i in range(3)]
        cs=[pltpu.roll(c[:,128*i:128*(i+1)],rot,1) for i in range(3)]
        keep=lane<128-sh
        for i in range(2):
            live=lane+128*i<n
            out[d,:,128*i:128*(i+1)]=jnp.where(live,jnp.where(keep,rs[i],rs[i+1]),0.)
            w=jnp.where(live,jnp.where(keep,cs[i],cs[i+1]),-1.)
            cells[d,:,128*i:128*(i+1)]=w[0:1]
        return _
    lax.fori_loop(0,128,expand,0,unroll=8)


def split(x):
    h=x.astype(BF); return h,(x-h.astype(F32)).astype(BF)
def weights(t):
    return 0.5*t*(t-1.), 1.-t*t, 0.5*t*(t+1.)
def setup(vel, halo, fh, fl, tab, masks):
    mu,md,ml,mr=masks
    lane=lax.broadcasted_iota(I32,(1,128),1)
    z8=jnp.zeros((8,256),F32)
    for c in range(2):
        ft=jnp.transpose(vel[c])
        lrow=halo[2][c:c+1,:]*ml
        rrow=halo[3][c:c+1,:]*mr
        e=jnp.concatenate([lrow,ft,rrow,jnp.zeros((6,256),F32)],axis=0)
        h,l=split(e)
        fh[c*136:(c+1)*136]=h; fl[c*136:(c+1)*136]=l
        rows=[]
        for (mid,lc,rc,m) in ((0,4,5,mu),(1,6,7,md)):
            r=halo[mid][c:c+1,:128]*m
            le=halo[lc][c:c+1,:128]*(m*ml); re=halo[rc][c:c+1,:128]*(m*mr)
            rows.append(jnp.where(lane==0,pltpu.roll(le,1,1),pltpu.roll(r,1,1)))
            rows.append(r)
            rows.append(jnp.where(lane==127,pltpu.roll(re,127,1),pltpu.roll(r,127,1)))
        tab[c]=jnp.concatenate(rows+[jnp.zeros((2,128),F32)],axis=0)
def interp(v, cell, fh, fl, tab):
    n=v.shape[1]
    zero=jnp.zeros((),BF)
    f=v[0:1]; g=v[1:2]
    live=cell>=0.
    cm=jnp.maximum(cell,0.)
    a=jnp.floor(cm*(1/128)); b=cm-128.*a
    wf=weights(f); wg=weights(g)
    ga=jnp.floor((a-1.)*(1/16)); oa=(a-1.)-16.*ga
    gab=jnp.broadcast_to(ga.astype(BF),(16,n))
    d=lax.broadcasted_iota(I32,(16,n),0).astype(F32).astype(BF)-jnp.broadcast_to(oa.astype(BF),(16,n))
    hl=[split(w) for w in wf]
    m0=d==0;m1=d==1;m2=d==2;q1=d==-15;q2=d==-14
    pats=[]
    for i in range(2):
        w=[jnp.broadcast_to(x[i],(16,n)) for x in hl]
        pats.append((jnp.where(m0,w[0],jnp.where(m1,w[1],jnp.where(m2,w[2],zero))),
                     jnp.where(q1,w[1],jnp.where(q2,w[2],zero))))
    ms=[gab==float(G) for G in range(-1,16)]
    W=[jnp.concatenate([jnp.where(ms[G+1],pa,jnp.where(ms[G],pb,zero)) for G in range(16)],axis=0) for pa,pb in pats]
    H=fh[...]; L=fl[...]
    R=dotf(H,W[0])+dotf(L,W[0])+dotf(H,W[1])
    gb=jnp.floor(b*(1/8)); ob=b-8.*gb
    gbb=jnp.broadcast_to(gb,(8,n))
    s8=lax.broadcasted_iota(I32,(8,n),0).astype(F32)
    d8=s8-ob
    pa=jnp.where(d8==0,wg[0],jnp.where(d8==1,wg[1],jnp.where(d8==2,wg[2],0.)))
    pb=jnp.where(d8==-7,wg[1],jnp.where(d8==-6,wg[2],0.))
    accA=[jnp.zeros((8,n),F32)]*2; accB=[jnp.zeros((8,n),F32)]*2
    mprev=None
    for G in range(17):
        m=gbb==float(G) if G<16 else None
        for c in range(2):
            r=R[c*136+8*G:c*136+8*G+8]
            if m is not None: accA[c]=jnp.where(m,r,accA[c])
            if mprev is not None: accB[c]=jnp.where(mprev,r,accB[c])
        mprev=m
    si=lax.broadcasted_iota(I32,(8,n),0)
    wj=jnp.where((si==0)|(si==3),wg[0],jnp.where((si==1)|(si==4),wg[1],wg[2]))
    up=jnp.where(a==0.,wf[0],0.); dn=jnp.where(a==255.,wf[2],0.)
    Pm=jnp.where(si<3,up,jnp.where(si<6,dn,0.))*wj
    bi=jnp.broadcast_to(b.astype(I32),(8,n))
    out=v
    for c in range(2):
        T=tab[c]
        corr=jnp.concatenate([jnp.take_along_axis(T,bi[:,128*i:128*(i+1)],axis=1) for i in range(n//128)],axis=1)
        sp=jnp.sum(pa*accA[c]+pb*accB[c]+Pm*corr,axis=0,keepdims=True)
        disp=jnp.where(live,0.5*sp,0.)
        out=out+jnp.where(si==2+c,disp,0.)
    return out
U = 4


def place_of(p):
    return (p // 32, (p % 32) // 2, p % 2)


def bucket_edges(vel, part, dest, ca, cb, out, cells, edges, *scratch):
    for c in range(2):
        zeros = jnp.zeros((1, 128), F32)
        edges[0, c : c + 1, :] = jnp.concatenate([vel[c, 0:1, :], zeros], axis=1)
        edges[1, c : c + 1, :] = jnp.concatenate([vel[c, 255:256, :], zeros], axis=1)
        turned = jnp.transpose(vel[c])
        edges[2, c : c + 1, :] = turned[0:1]
        edges[3, c : c + 1, :] = turned[127:128]
    bucket(part, dest, ca, cb, out, cells, *scratch)


def exchange(vel, edges, send, scell, out, cout, recv, rcell, halo, fh, fl, tab, ss, ra, rb, rh):
    gx = lax.axis_index("gx")
    col = lax.axis_index("gy") * 2 + lax.axis_index("gz")
    me = gx * 32 + col
    barrier = pltpu.get_barrier_semaphore()

    def greet(k, _):
        p = lax.rem(me + k, 128)
        pl.semaphore_signal(barrier, inc=1, device_id=place_of(p), device_id_type=MESH)
        return _

    lax.fori_loop(1, 128, greet, 0)
    recv[me] = send[me]
    rcell[me] = scell[me]
    pl.semaphore_wait(barrier, 127)

    def neighbour(da, db):
        return lax.rem(gx + da + 4, 4) * 32 + lax.rem(col + db + 32, 32)

    sides = ((1, 0, 1, 0), (0, 1, -1, 0), (3, 2, 0, 1), (2, 3, 0, -1), (1, 4, 1, 1), (1, 5, 1, -1), (0, 6, -1, 1), (0, 7, -1, -1))
    borders = []
    for edge, slot, da, db in sides:
        borders.append(
            pltpu.make_async_remote_copy(
                src_ref=edges.at[edge],
                dst_ref=halo.at[slot],
                send_sem=ss.at[2],
                recv_sem=rh.at[slot],
                device_id=place_of(neighbour(da, db)),
                device_id_type=MESH,
            )
        )
    for copy in borders:
        copy.start()

    def ship(k, _):
        p = lax.rem(me + k, 128)
        group = k // U
        pltpu.make_async_remote_copy(
            src_ref=send.at[p], dst_ref=recv.at[me], send_sem=ss.at[0], recv_sem=ra.at[group],
            device_id=place_of(p), device_id_type=MESH).start()
        pltpu.make_async_remote_copy(
            src_ref=scell.at[p], dst_ref=rcell.at[me], send_sem=ss.at[1], recv_sem=rb.at[group],
            device_id=place_of(p), device_id_type=MESH).start()
        return _

    lax.fori_loop(1, 128, ship, 0)

    def bytes_of(n, src, dst, s_sem, r_sem):
        return pltpu.make_async_remote_copy(
            src_ref=src.at[pl.ds(0, n)], dst_ref=dst.at[pl.ds(0, n)], send_sem=s_sem, recv_sem=r_sem,
            device_id=place_of(lax.rem(me + 1, 128)), device_id_type=MESH)

    for copy in borders:
        copy.wait_recv()
    masks = [(gx > 0).astype(F32), (gx < 3).astype(F32), (col > 0).astype(F32), (col < 31).astype(F32)]
    setup(vel, halo, fh, fl, tab, masks)

    def group_of(i):
        for u in range(U):
            s = lax.rem(me - (i * U + u) + 128, 128)
            v = recv[s]
            cell = rcell[s]
            out[:, pl.ds(pl.multiple_of(s * 256, 256), 256)] = interp(v, cell, fh, fl, tab)
            cout[s] = cell.astype(I32)

    bytes_of(U - 1, send, recv, ss.at[0], ra.at[0]).wait_recv()
    bytes_of(U - 1, scell, rcell, ss.at[1], rb.at[0]).wait_recv()

    def step(i, _):
        group_of(i)

        @pl.when(i < 128 // U - 1)
        def _wait():
            bytes_of(U, send, recv, ss.at[0], ra.at[i + 1]).wait_recv()
            bytes_of(U, scell, rcell, ss.at[1], rb.at[i + 1]).wait_recv()

        return _

    lax.fori_loop(0, 128 // U, step, 0)
    bytes_of(127, send, recv, ss.at[0], ra.at[0]).wait_send()
    bytes_of(127, scell, rcell, ss.at[1], rb.at[0]).wait_send()
    bytes_of(8, halo, halo, ss.at[2], rh.at[0]).wait_send()


def vmem(n):
    return [pl.BlockSpec(memory_space=pltpu.VMEM)] * n


def shards(particles, dest_key, cell_a, cell_b, velocity):
    send, scell, edges = pl.pallas_call(
        bucket_edges,
        out_shape=(
            jax.ShapeDtypeStruct((128, 8, 256), F32),
            jax.ShapeDtypeStruct((128, 1, 256), F32),
            jax.ShapeDtypeStruct((4, 2, 256), F32),
        ),
        in_specs=vmem(5),
        out_specs=vmem(3),
        scratch_shapes=[
            pltpu.VMEM((32, 128, 256), BF),
            pltpu.VMEM((8, 8704), F32),
            pltpu.VMEM((8, 8704), F32),
            pltpu.VMEM((576, 256), F32),
            pltpu.VMEM((8, 128), I32),
            pltpu.SMEM((8, 128), I32),
            pltpu.SemaphoreType.DMA,
        ],
        name="bucket",
    )(velocity, particles, dest_key.reshape(64, 128), cell_a.reshape(64, 128), cell_b.reshape(64, 128))
    binned, cells = pl.pallas_call(
        exchange,
        out_shape=(jax.ShapeDtypeStruct((8, 32768), F32), jax.ShapeDtypeStruct((128, 1, 256), I32)),
        in_specs=vmem(4),
        out_specs=vmem(2),
        scratch_shapes=[
            pltpu.VMEM((128, 8, 256), F32),
            pltpu.VMEM((128, 1, 256), F32),
            pltpu.VMEM((8, 2, 256), F32),
            pltpu.VMEM((272, 256), BF),
            pltpu.VMEM((272, 256), BF),
            pltpu.VMEM((2, 8, 128), F32),
            pltpu.SemaphoreType.DMA((3,)),
            pltpu.SemaphoreType.DMA((128 // U,)),
            pltpu.SemaphoreType.DMA((128 // U,)),
            pltpu.SemaphoreType.DMA((8,)),
        ],
        compiler_params=pltpu.CompilerParams(collective_id=0, has_side_effects=True),
        name="exchange",
    )(velocity, edges, send, scell)
    return binned, cells.reshape(-1)


def solution(mesh):
    in_specs = (P(None, AXES), P(AXES), P(AXES), P(AXES), P(None, "gx", ("gy", "gz")))
    return jax.shard_map(
        shards, mesh=mesh, in_specs=in_specs, out_specs=(P(None, AXES), P(AXES)), check_vma=False
    )
```

```python
import jax
import jax.numpy as jnp
from jax import lax
from jax.experimental import pallas as pl
from jax.experimental.pallas import tpu as pltpu
from jax.sharding import PartitionSpec as P

BF = jnp.bfloat16
F32 = jnp.float32
I32 = jnp.int32
NT = (((1,), (1,)), ((), ()))
AXES = ("gx", "gy", "gz")
LOGICAL = pl.DeviceIdType.LOGICAL
SIDES = ((1, 1, 0), (0, -1, 0), (3, 0, 1), (2, 0, -1), (1, 1, 1), (1, 1, -1), (0, -1, 1), (0, -1, -1))


def dotf(a, b):
    return jnp.dot(a, b, preferred_element_type=F32)


PB=8
UB=8
XB=16
U=16

def row256(ref, j):
    r = ref[pl.ds(2*j,2),:]
    return jnp.concatenate([r[0:1],r[1:2]],axis=1)

def bucket(part, dest, ca, cb, out, oh, pos_s, srt, csrt, acc, stv, sts, sem, first):
    nb=32
    one=jnp.ones((),BF); zero=jnp.zeros((),BF)
    iod=lax.broadcasted_iota(I32,(128,256),0).astype(F32).astype(BF)
    def onehot(j,S):
        d=row256(dest,j).astype(F32).astype(BF)
        o=jnp.where(iod==jnp.broadcast_to(d,(128,256)),one,zero)
        oh[j]=o
        return S+o
    S=lax.fori_loop(0,nb,onehot,jnp.zeros((128,256),BF),unroll=4)
    ones=jnp.ones((256,256),BF)
    tot=dotf(S,ones)
    low=(lax.broadcasted_iota(I32,(128,128),0)>lax.broadcasted_iota(I32,(128,128),1)).astype(F32).astype(BF)
    start=dotf(low,tot.astype(BF))
    diag=lax.broadcasted_iota(I32,(128,128),0)==lax.broadcasted_iota(I32,(128,128),1)
    srow=jnp.sum(jnp.where(diag,start[:,:128],0.),axis=0,keepdims=True)
    trow=jnp.sum(jnp.where(diag,tot[:,:128],0.),axis=0,keepdims=True)
    tile=jnp.floor(srow*(1/128))
    sh=srow-128.*tile
    stv[0:1,:]=tile.astype(I32)
    stv[1:2,:]=jnp.where(sh==0.,0.,128.-sh).astype(I32)
    stv[2:3,:]=(128.-sh).astype(I32)
    stv[3:4,:]=trow.astype(I32)
    cp=pltpu.make_async_copy(stv,sts,sem)
    cp.start()
    up=(lax.broadcasted_iota(I32,(256,256),0)<lax.broadcasted_iota(I32,(256,256),1)).astype(F32).astype(BF)
    upones=jnp.concatenate([up,ones],axis=0)
    lane=lax.broadcasted_iota(I32,(128,256),1).astype(F32)
    C0=jnp.floor((start+255.-lane)*(1/256)).astype(BF)
    def ranks(jj,C):
        for u in range(PB):
            j=jj*PB+u
            o=oh[j]
            x=dotf(jnp.concatenate([o,C],axis=1),upones)
            pos=jnp.sum(o.astype(F32)*x,axis=0,keepdims=True)
            hi=jnp.floor(pos*(1/256))
            pos_s[j,0:1,:]=hi
            pos_s[j,1:2,:]=pos-256.*hi
            C=C+o
        return C
    lax.fori_loop(0,nb//PB,ranks,C0)
    acc[...]=jnp.zeros_like(acc)
    iol=lax.broadcasted_iota(I32,(256,256),0).astype(F32).astype(BF)
    s16=lax.broadcasted_iota(I32,(16,256),0)
    half=(s16//8).astype(F32).astype(BF)
    i32_=lax.broadcasted_iota(I32,(32,256),0).astype(F32).astype(BF)
    def place(jj,_):
        As=[];Ls=[]
        for u in range(UB):
            j=jj*UB+u
            hi=pos_s[j,0:1,:].astype(BF); lo=pos_s[j,1:2,:].astype(BF)
            lot=jnp.where(iol==jnp.broadcast_to(lo,(256,256)),one,zero)
            v=part[:,pl.ds(pl.multiple_of(j*256,256),256)]
            vh=v.astype(BF).astype(F32); vl=v-vh
            vh2=jnp.concatenate([vh,vh],axis=0).astype(BF)
            vl2=jnp.concatenate([vl,vl],axis=0).astype(BF)
            h16=jnp.broadcast_to(hi,(16,256))-half
            hs=[];ls=[]
            for k in range(16):
                m=h16==float(2*k)
                hs.append(jnp.where(m,vh2,zero)); ls.append(jnp.where(m,vl2,zero))
            m32=i32_==jnp.broadcast_to(hi,(32,256))
            a=row256(ca,j).astype(F32).astype(BF); b=row256(cb,j).astype(F32).astype(BF)
            As.append(jnp.concatenate(hs+ls+[jnp.where(m32,jnp.broadcast_to(a,(32,256)),zero),jnp.where(m32,jnp.broadcast_to(b,(32,256)),zero)],axis=0))
            Ls.append(lot)
        acc[...]+=lax.dot_general(jnp.concatenate(As,axis=1),jnp.concatenate(Ls,axis=1),NT,preferred_element_type=F32)
        return _
    lax.fori_loop(0,nb//UB,place,0)
    for h in range(32):
        x=acc[h*8:(h+1)*8]+acc[256+h*8:256+(h+1)*8]
        srt[2*h]=x[:,:128]; srt[2*h+1]=x[:,128:]
    cc=acc[512:544]*128.+acc[544:576]
    for t in range(64):
        r=cc[t//2:t//2+1,(t%2)*128:(t%2)*128+128]
        for i in range(3):
            if t-i>=0: csrt[t-i,i:i+1,:]=r
    cp.wait()
    lane=lax.broadcasted_iota(I32,(8,128),1)
    sub=lax.broadcasted_iota(I32,(8,128),0)
    place256=lane+128*sub
    def expand(dd,_):
        e=first+dd
        e=jnp.where(e>=128//XB,e-128//XB,e)
        for u in range(XB):
            d=e*XB+u
            t=jnp.clip(sts[0,d],0,64); rot=sts[1,d]; thr=sts[2,d]; n=sts[3,d]
            rs=[pltpu.roll(srt[t+i],rot,1) for i in range(3)]
            c=pltpu.roll(csrt[t],rot,1)
            keep=lane<thr
            for i in range(2):
                out[d,i]=jnp.where(lane<n-128*i,jnp.where(keep,rs[i],rs[i+1]),0.)
            out[d,2]=jnp.where(place256<n,jnp.where(keep,c,pltpu.roll(c,7,0)),-1.)
        return _
    lax.fori_loop(0,128//XB,expand,0)

def split(x):
    h=x.astype(BF); return h,(x-h.astype(F32)).astype(BF)
def weights(t):
    return 0.5*t*(t-1.), 1.-t*t, 0.5*t*(t+1.)
def setup(vel, halo, fh, fl, tab, masks):
    mu,md,ml,mr=masks
    lane=lax.broadcasted_iota(I32,(1,128),1)
    z8=jnp.zeros((8,256),F32)
    for c in range(2):
        ft=jnp.transpose(vel[c])
        lrow=halo[2][c:c+1,:]*ml
        rrow=halo[3][c:c+1,:]*mr
        e=jnp.concatenate([lrow,ft,rrow,jnp.zeros((6,256),F32)],axis=0)
        h,l=split(e)
        fh[c*136:(c+1)*136]=h; fl[c*136:(c+1)*136]=l
        rows=[]
        for (mid,lc,rc,m) in ((0,4,5,mu),(1,6,7,md)):
            r=halo[mid][c:c+1,:128]*m
            le=halo[lc][c:c+1,:128]*(m*ml); re=halo[rc][c:c+1,:128]*(m*mr)
            rows.append(jnp.where(lane==0,pltpu.roll(le,1,1),pltpu.roll(r,1,1)))
            rows.append(r)
            rows.append(jnp.where(lane==127,pltpu.roll(re,127,1),pltpu.roll(r,127,1)))
        tab[c]=jnp.concatenate(rows+[jnp.zeros((2,128),F32)],axis=0)
def cellparts(cell):
    cm=jnp.maximum(cell,0.)
    a=jnp.floor(cm*(1/128)); b=cm-128.*a
    return a,b
def pick(rows, bits):
    level=list(rows)
    for m in bits:
        level=[jnp.where(m,level[2*k+1],level[2*k]) for k in range(len(level)//2)]
    return level[0]
def interp(v, cell, fh, fl, tab):
    n=v.shape[1]
    zero=jnp.zeros((),BF)
    f=v[0:1]; g=v[1:2]
    live=cell>=0.
    a,b=cellparts(cell)
    wf=weights(f); wg=weights(g)
    ga=jnp.floor((a-1.)*(1/16)); oa=(a-1.)-16.*ga
    gab=jnp.broadcast_to(ga.astype(BF),(16,n))
    d=lax.broadcasted_iota(I32,(16,n),0).astype(F32).astype(BF)-jnp.broadcast_to(oa.astype(BF),(16,n))
    hl=[split(w) for w in wf]
    m0=d==0;m1=d==1;m2=d==2;q1=d==-15;q2=d==-14
    pats=[]
    for i in range(2):
        w=[jnp.broadcast_to(x[i],(16,n)) for x in hl]
        pats.append((jnp.where(m0,w[0],jnp.where(m1,w[1],jnp.where(m2,w[2],zero))),
                     jnp.where(q1,w[1],jnp.where(q2,w[2],zero))))
    ms=[gab==float(G) for G in range(-1,16)]
    W=[jnp.concatenate([jnp.where(ms[G+1],pa,jnp.where(ms[G],pb,zero)) for G in range(16)],axis=0) for pa,pb in pats]
    H=fh[...]; L=fl[...]
    R=dotf(H,W[0])+dotf(L,W[0])+dotf(H,W[1])
    gb=jnp.floor(b*(1/8)); ob=b-8.*gb
    s8=lax.broadcasted_iota(I32,(8,n),0).astype(F32)
    d8=s8-ob
    pa=jnp.where(d8==0,wg[0],jnp.where(d8==1,wg[1],jnp.where(d8==2,wg[2],0.)))
    pb=jnp.where(d8==-7,wg[1],jnp.where(d8==-6,wg[2],0.))
    gi=jnp.broadcast_to(gb,(8,n)).astype(I32)
    bits=[(gi&(1<<k))!=0 for k in range(4)]
    accs=[]
    for c in range(2):
        rows=[R[c*136+8*G:c*136+8*G+8] for G in range(17)]
        accs.append((pick(rows[:16],bits),pick(rows[1:],bits)))
    si=lax.broadcasted_iota(I32,(8,n),0)
    wj=jnp.where((si==0)|(si==3),wg[0],jnp.where((si==1)|(si==4),wg[1],wg[2]))
    up=jnp.where(a==0.,wf[0],0.); dn=jnp.where(a==255.,wf[2],0.)
    Pm=jnp.where(si<3,up,jnp.where(si<6,dn,0.))*wj
    bi=jnp.broadcast_to(b.astype(I32),(8,n))
    out=v
    for c in range(2):
        T=tab[c]
        corr=jnp.concatenate([jnp.take_along_axis(T,bi[:,128*i:128*(i+1)],axis=1) for i in range(n//128)],axis=1)
        sp=jnp.sum(pa*accs[c][0]+pb*accs[c][1]+Pm*corr,axis=0,keepdims=True)
        disp=jnp.where(live,0.5*sp,0.)
        out=out+jnp.where(si==2+c,disp,0.)
    return out


def fused(vel, part, dest, ca, cb, out, cout, send, recv, edges, halo, fh, fl, tab, oh, pos_s, srt, csrt, acc, stv, sts, sem, ss, ra, rh):
    gx = lax.axis_index("gx")
    col = lax.axis_index("gy") * 2 + lax.axis_index("gz")
    me = gx * 32 + col
    barrier = pltpu.get_barrier_semaphore()

    def other(k):
        p = me + k
        return jnp.where(p >= 128, p - 128, p)

    def greet(k, _):
        pl.semaphore_signal(barrier, inc=1, device_id=other(k), device_id_type=LOGICAL)
        return _

    lax.fori_loop(1, 128, greet, 0)
    for c in range(2):
        zeros = jnp.zeros((1, 128), F32)
        edges[0, c : c + 1, :] = jnp.concatenate([vel[c, 0:1, :], zeros], axis=1)
        edges[1, c : c + 1, :] = jnp.concatenate([vel[c, 255:256, :], zeros], axis=1)
        turned = jnp.transpose(vel[c])
        edges[2, c : c + 1, :] = turned[0:1]
        edges[3, c : c + 1, :] = turned[127:128]
    bucket(part, dest, ca, cb, send, oh, pos_s, srt, csrt, acc, stv, sts, sem, me // XB)
    recv[me] = send[me]
    pl.semaphore_wait(barrier, 127)

    def neighbour(da, db):
        return lax.rem(gx + da + 4, 4) * 32 + lax.rem(col + db + 32, 32)

    borders = []
    for slot, (edge, da, db) in enumerate(SIDES):
        borders.append(
            pltpu.make_async_remote_copy(
                src_ref=edges.at[edge],
                dst_ref=halo.at[slot],
                send_sem=ss.at[1],
                recv_sem=rh.at[slot],
                device_id=neighbour(da, db),
                device_id_type=LOGICAL,
            )
        )
    for copy in borders:
        copy.start()

    for group in range(128 // U):

        def ship(k, _):
            p = other(k)
            pltpu.make_async_remote_copy(
                src_ref=send.at[p],
                dst_ref=recv.at[me],
                send_sem=ss.at[0],
                recv_sem=ra.at[group],
                device_id=p,
                device_id_type=LOGICAL,
            ).start()
            return _

        lax.fori_loop(max(1, group * U), group * U + U, ship, 0)

    def bytes_of(n, r_sem):
        return pltpu.make_async_remote_copy(
            src_ref=send.at[pl.ds(0, n)],
            dst_ref=recv.at[pl.ds(0, n)],
            send_sem=ss.at[0],
            recv_sem=r_sem,
            device_id=other(1),
            device_id_type=LOGICAL,
        )

    for copy in borders:
        copy.wait_recv()
    masks = [(gx > 0).astype(F32), (gx < 3).astype(F32), (col > 0).astype(F32), (col < 31).astype(F32)]
    setup(vel, halo, fh, fl, tab, masks)
    bytes_of(U - 1, ra.at[0]).wait_recv()

    def step(i, _):
        for u in range(U):
            s = me - (i * U + u)
            s = jnp.where(s < 0, s + 128, s)
            block = recv[s]
            v = jnp.concatenate([block[0], block[1]], axis=1)
            cell = jnp.concatenate([block[2, 0:1], block[2, 1:2]], axis=1)
            out[:, pl.ds(pl.multiple_of(s * 256, 256), 256)] = interp(v, cell, fh, fl, tab)
            cout[s] = cell.astype(I32)

        @pl.when(i < 128 // U - 1)
        def _wait():
            bytes_of(U, ra.at[i + 1]).wait_recv()

        return _

    lax.fori_loop(0, 128 // U, step, 0)
    bytes_of(127, ra.at[0]).wait_send()
    pltpu.make_async_remote_copy(
        src_ref=halo, dst_ref=halo, send_sem=ss.at[1], recv_sem=rh.at[0], device_id=other(1), device_id_type=LOGICAL
    ).wait_send()


def shards(particles, dest_key, cell_a, cell_b, velocity):
    vmem = pl.BlockSpec(memory_space=pltpu.VMEM)
    binned, cells = pl.pallas_call(
        fused,
        out_shape=(jax.ShapeDtypeStruct((8, 32768), F32), jax.ShapeDtypeStruct((128, 1, 256), I32)),
        in_specs=[vmem] * 5,
        out_specs=[vmem] * 2,
        scratch_shapes=[
            pltpu.VMEM((128, 3, 8, 128), F32),
            pltpu.VMEM((128, 3, 8, 128), F32),
            pltpu.VMEM((4, 2, 256), F32),
            pltpu.VMEM((8, 2, 256), F32),
            pltpu.VMEM((272, 256), BF),
            pltpu.VMEM((272, 256), BF),
            pltpu.VMEM((2, 8, 128), F32),
            pltpu.VMEM((32, 128, 256), BF),
            pltpu.VMEM((32, 2, 256), F32),
            pltpu.VMEM((67, 8, 128), F32),
            pltpu.VMEM((67, 8, 128), F32),
            pltpu.VMEM((576, 256), F32),
            pltpu.VMEM((8, 128), I32),
            pltpu.SMEM((8, 128), I32),
            pltpu.SemaphoreType.DMA,
            pltpu.SemaphoreType.DMA((2,)),
            pltpu.SemaphoreType.DMA((128 // U,)),
            pltpu.SemaphoreType.DMA((8,)),
        ],
        compiler_params=pltpu.CompilerParams(collective_id=0, has_side_effects=True),
        name="rebin",
    )(velocity, particles, dest_key.reshape(64, 128), cell_a.reshape(64, 128), cell_b.reshape(64, 128))
    return binned, cells.reshape(-1)


def solution(mesh):
    in_specs = (P(None, AXES), P(AXES), P(AXES), P(AXES), P(None, "gx", ("gy", "gz")))
    return jax.shard_map(
        shards, mesh=mesh, in_specs=in_specs, out_specs=(P(None, AXES), P(AXES)), check_vma=False
    )
```

```python
import jax
import jax.numpy as jnp
from jax import lax
from jax.experimental import pallas as pl
from jax.experimental.pallas import tpu as pltpu
from jax.sharding import PartitionSpec as P

BF = jnp.bfloat16
F32 = jnp.float32
I32 = jnp.int32
NT = (((1,), (1,)), ((), ()))
AXES = ("gx", "gy", "gz")
LOGICAL = pl.DeviceIdType.LOGICAL
SIDES = ((1, 1, 0), (0, -1, 0), (3, 0, 1), (2, 0, -1), (1, 1, 1), (1, 1, -1), (0, -1, 1), (0, -1, -1))


def dotf(a, b):
    return jnp.dot(a, b, preferred_element_type=F32)


PB=8
UB=8
XB=16
U=16
STRIDE=27

def row256(ref, j):
    r = ref[pl.ds(2*j,2),:]
    return jnp.concatenate([r[0:1],r[1:2]],axis=1)

def bucket(part, dest, ca, cb, out, cells, oh, pos_s, srt, csrt, acc, stv, sts, sem, target, turn, ship, ready, open_links):
    nb=32
    one=jnp.ones((),BF); zero=jnp.zeros((),BF)
    iod=lax.broadcasted_iota(I32,(128,256),0).astype(F32).astype(BF)
    def onehot(j,S):
        d=row256(dest,j).astype(F32).astype(BF)
        o=jnp.where(iod==jnp.broadcast_to(d,(128,256)),one,zero)
        oh[j]=o
        return S+o
    S=lax.fori_loop(0,nb,onehot,jnp.zeros((128,256),BF),unroll=4)
    ones=jnp.ones((256,256),BF)
    tot=dotf(S,ones)
    low=(lax.broadcasted_iota(I32,(128,128),0)>lax.broadcasted_iota(I32,(128,128),1)).astype(F32).astype(BF)
    start=dotf(low,tot.astype(BF))
    diag=lax.broadcasted_iota(I32,(128,128),0)==lax.broadcasted_iota(I32,(128,128),1)
    srow=jnp.sum(jnp.where(diag,start[:,:128],0.),axis=0,keepdims=True)
    trow=jnp.sum(jnp.where(diag,tot[:,:128],0.),axis=0,keepdims=True)
    tile=jnp.floor(srow*(1/128))
    sh=srow-128.*tile
    stv[0:1,:]=tile.astype(I32)
    stv[1:2,:]=jnp.where(sh==0.,0.,128.-sh).astype(I32)
    stv[2:3,:]=(128.-sh).astype(I32)
    stv[3:4,:]=trow.astype(I32)
    cp=pltpu.make_async_copy(stv,sts,sem)
    cp.start()
    up=(lax.broadcasted_iota(I32,(256,256),0)<lax.broadcasted_iota(I32,(256,256),1)).astype(F32).astype(BF)
    upones=jnp.concatenate([up,ones],axis=0)
    lane=lax.broadcasted_iota(I32,(128,256),1).astype(F32)
    C0=jnp.floor((start+255.-lane)*(1/256)).astype(BF)
    def ranks(jj,C):
        for u in range(PB):
            j=jj*PB+u
            o=oh[j]
            x=dotf(jnp.concatenate([o,C],axis=1),upones)
            pos=jnp.sum(o.astype(F32)*x,axis=0,keepdims=True)
            hi=jnp.floor(pos*(1/256))
            pos_s[j,0:1,:]=hi
            pos_s[j,1:2,:]=pos-256.*hi
            C=C+o
        return C
    lax.fori_loop(0,nb//PB,ranks,C0)
    acc[...]=jnp.zeros_like(acc)
    ready()
    iol=lax.broadcasted_iota(I32,(256,256),0).astype(F32).astype(BF)
    s16=lax.broadcasted_iota(I32,(16,256),0)
    half=(s16//8).astype(F32).astype(BF)
    i32_=lax.broadcasted_iota(I32,(32,256),0).astype(F32).astype(BF)
    def place(jj,_):
        As=[];Ls=[]
        for u in range(UB):
            j=jj*UB+u
            hi=pos_s[j,0:1,:].astype(BF); lo=pos_s[j,1:2,:].astype(BF)
            lot=jnp.where(iol==jnp.broadcast_to(lo,(256,256)),one,zero)
            v=part[:,pl.ds(pl.multiple_of(j*256,256),256)]
            vh=v.astype(BF).astype(F32); vl=v-vh
            vh2=jnp.concatenate([vh,vh],axis=0).astype(BF)
            vl2=jnp.concatenate([vl,vl],axis=0).astype(BF)
            h16=jnp.broadcast_to(hi,(16,256))-half
            hs=[];ls=[]
            for k in range(16):
                m=h16==float(2*k)
                hs.append(jnp.where(m,vh2,zero)); ls.append(jnp.where(m,vl2,zero))
            m32=i32_==jnp.broadcast_to(hi,(32,256))
            a=row256(ca,j).astype(F32).astype(BF); b=row256(cb,j).astype(F32).astype(BF)
            As.append(jnp.concatenate(hs+ls+[jnp.where(m32,jnp.broadcast_to(a,(32,256)),zero),jnp.where(m32,jnp.broadcast_to(b,(32,256)),zero)],axis=0))
            Ls.append(lot)
        acc[...]+=lax.dot_general(jnp.concatenate(As,axis=1),jnp.concatenate(Ls,axis=1),NT,preferred_element_type=F32)
        return _
    lax.fori_loop(0,nb//UB,place,0)
    for h in range(32):
        x=acc[h*8:(h+1)*8]+acc[256+h*8:256+(h+1)*8]
        srt[2*h]=x[:,:128]; srt[2*h+1]=x[:,128:]
    cc=acc[512:544]*128.+acc[544:576]
    for t in range(64):
        r=cc[t//2:t//2+1,(t%2)*128:(t%2)*128+128]
        for i in range(3):
            if t-i>=0: csrt[t-i,i:i+1,:]=r
    cp.wait()
    lane=lax.broadcasted_iota(I32,(8,128),1)
    def expand(k):
        d=target(k)
        t=jnp.clip(sts[0,d],0,64); rot=sts[1,d]; thr=sts[2,d]; n=sts[3,d]
        rs=[pltpu.roll(srt[t+i],rot,1) for i in range(3)]
        c=pltpu.roll(csrt[t],rot,1)
        keep=lane<thr
        c1=jnp.where(keep[0:2],c[0:2],c[1:3])
        for i in range(2):
            live=lane<n-128*i
            out[d,:,128*i:128*(i+1)]=jnp.where(live,jnp.where(keep,rs[i],rs[i+1]),0.)
            cells[d,:,128*i:128*(i+1)]=jnp.where(live[0:1],c1[i:i+1],-1.)
    def back(k):
        k=k-STRIDE*XB%128
        return jnp.where(k<0,k+128,k)
    def deliver(i,k):
        old=k
        for u in range(XB):
            k=turn(k)
            expand(k)
        @pl.when(i>0)
        def _():
            ship(i-1,back(old),XB)
        return k
    open_links()
    k=lax.fori_loop(0,128//XB,deliver,0)
    ship(128//XB-1,back(k),XB-1)

def split(x):
    h=x.astype(BF); return h,(x-h.astype(F32)).astype(BF)
def weights(t):
    return 0.5*t*(t-1.), 1.-t*t, 0.5*t*(t+1.)
def setup(vel, halo, fh, fl, tab, masks):
    mu,md,ml,mr=masks
    lane=lax.broadcasted_iota(I32,(1,128),1)
    z8=jnp.zeros((8,256),F32)
    for c in range(2):
        ft=jnp.transpose(vel[c])
        lrow=halo[2][c:c+1,:]*ml
        rrow=halo[3][c:c+1,:]*mr
        e=jnp.concatenate([lrow,ft,rrow,jnp.zeros((6,256),F32)],axis=0)
        h,l=split(e)
        fh[c*136:(c+1)*136]=h; fl[c*136:(c+1)*136]=l
        rows=[]
        for (mid,lc,rc,m) in ((0,4,5,mu),(1,6,7,md)):
            r=halo[mid][c:c+1,:128]*m
            le=halo[lc][c:c+1,:128]*(m*ml); re=halo[rc][c:c+1,:128]*(m*mr)
            rows.append(jnp.where(lane==0,pltpu.roll(le,1,1),pltpu.roll(r,1,1)))
            rows.append(r)
            rows.append(jnp.where(lane==127,pltpu.roll(re,127,1),pltpu.roll(r,127,1)))
        tab[c]=jnp.concatenate(rows+[jnp.zeros((2,128),F32)],axis=0)
def cellparts(cell):
    cm=jnp.maximum(cell,0.)
    a=jnp.floor(cm*(1/128)); b=cm-128.*a
    return a,b
def pick(rows, bits):
    level=list(rows)
    for m in bits:
        level=[jnp.where(m,level[2*k+1],level[2*k]) for k in range(len(level)//2)]
    return level[0]
def interp(v, cell, fh, fl, tab):
    n=v.shape[1]
    zero=jnp.zeros((),BF)
    f=v[0:1]; g=v[1:2]
    live=cell>=0.
    a,b=cellparts(cell)
    wf=weights(f); wg=weights(g)
    ga=jnp.floor((a-1.)*(1/16)); oa=(a-1.)-16.*ga
    gab=jnp.broadcast_to(ga.astype(BF),(16,n))
    d=lax.broadcasted_iota(I32,(16,n),0).astype(F32).astype(BF)-jnp.broadcast_to(oa.astype(BF),(16,n))
    hl=[split(w) for w in wf]
    m0=d==0;m1=d==1;m2=d==2;q1=d==-15;q2=d==-14
    pats=[]
    for i in range(2):
        w=[jnp.broadcast_to(x[i],(16,n)) for x in hl]
        pats.append((jnp.where(m0,w[0],jnp.where(m1,w[1],jnp.where(m2,w[2],zero))),
                     jnp.where(q1,w[1],jnp.where(q2,w[2],zero))))
    ms=[gab==float(G) for G in range(-1,16)]
    W=[jnp.concatenate([jnp.where(ms[G+1],pa,jnp.where(ms[G],pb,zero)) for G in range(16)],axis=0) for pa,pb in pats]
    H=fh[...]; L=fl[...]
    R=dotf(H,W[0])+dotf(L,W[0])+dotf(H,W[1])
    gb=jnp.floor(b*(1/8)); ob=b-8.*gb
    s8=lax.broadcasted_iota(I32,(8,n),0).astype(F32)
    d8=s8-ob
    pa=jnp.where(d8==0,wg[0],jnp.where(d8==1,wg[1],jnp.where(d8==2,wg[2],0.)))
    pb=jnp.where(d8==-7,wg[1],jnp.where(d8==-6,wg[2],0.))
    gi=jnp.broadcast_to(gb,(8,n)).astype(I32)
    bits=[(gi&(1<<k))!=0 for k in range(4)]
    accs=[]
    for c in range(2):
        rows=[R[c*136+8*G:c*136+8*G+8] for G in range(17)]
        accs.append((pick(rows[:16],bits),pick(rows[1:],bits)))
    si=lax.broadcasted_iota(I32,(8,n),0)
    wj=jnp.where((si==0)|(si==3),wg[0],jnp.where((si==1)|(si==4),wg[1],wg[2]))
    up=jnp.where(a==0.,wf[0],0.); dn=jnp.where(a==255.,wf[2],0.)
    Pm=jnp.where(si<3,up,jnp.where(si<6,dn,0.))*wj
    bi=jnp.broadcast_to(b.astype(I32),(8,n))
    out=v
    for c in range(2):
        T=tab[c]
        corr=jnp.concatenate([jnp.take_along_axis(T,bi[:,128*i:128*(i+1)],axis=1) for i in range(n//128)],axis=1)
        sp=jnp.sum(pa*accs[c][0]+pb*accs[c][1]+Pm*corr,axis=0,keepdims=True)
        disp=jnp.where(live,0.5*sp,0.)
        out=out+jnp.where(si==2+c,disp,0.)
    return out


def fused(vel_in, part_in, dest_in, ca_in, cb_in, out, cout, vel, part, dest, ca, cb, send, scell, recv, rcell, edges, halo,
          fh, fl, tab, oh, pos_s, srt, csrt, acc, stv, sts, sem, ins, ss, ra, rb, rh):
    loads = [
        pltpu.make_async_copy(src, dst, ins.at[i])
        for i, (src, dst) in enumerate(((dest_in, dest), (vel_in, vel), (ca_in, ca), (cb_in, cb), (part_in, part)))
    ]
    for load in loads:
        load.start()
    gx = lax.axis_index("gx")
    col = lax.axis_index("gy") * 2 + lax.axis_index("gz")
    me = gx * 32 + col
    barrier = pltpu.get_barrier_semaphore()

    def wrap(p):
        return jnp.where(p >= 128, p - 128, p)

    def other(k):
        return wrap(me + k)

    def turn(k):
        return wrap(k + STRIDE)

    def greet(k, _):
        pl.semaphore_signal(barrier, inc=1, device_id=other(k), device_id_type=LOGICAL)
        return _

    lax.fori_loop(1, 128, greet, 0)
    loads[0].wait()
    loads[1].wait()
    for c in range(2):
        zeros = jnp.zeros((1, 128), F32)
        edges[0, c : c + 1, :] = jnp.concatenate([vel[c, 0:1, :], zeros], axis=1)
        edges[1, c : c + 1, :] = jnp.concatenate([vel[c, 255:256, :], zeros], axis=1)
        turned = jnp.transpose(vel[c])
        edges[2, c : c + 1, :] = turned[0:1]
        edges[3, c : c + 1, :] = turned[127:128]

    def neighbour(da, db):
        return lax.rem(gx + da + 4, 4) * 32 + lax.rem(col + db + 32, 32)

    borders = []
    for slot, (edge, da, db) in enumerate(SIDES):
        borders.append(
            pltpu.make_async_remote_copy(
                src_ref=edges.at[edge],
                dst_ref=halo.at[slot],
                send_sem=ss.at[2],
                recv_sem=rh.at[slot],
                device_id=neighbour(da, db),
                device_id_type=LOGICAL,
            )
        )

    def ready():
        for load in loads[2:]:
            load.wait()

    def ship(group, k, count):
        for u in range(count):
            k = turn(k)
            p = other(k)
            for src, dst, lane_sem, done in ((send, recv, ss.at[0], ra), (scell, rcell, ss.at[1], rb)):
                pltpu.make_async_remote_copy(
                    src_ref=src.at[p],
                    dst_ref=dst.at[me],
                    send_sem=lane_sem,
                    recv_sem=done.at[group],
                    device_id=p,
                    device_id_type=LOGICAL,
                ).start()

    def open_links():
        pl.semaphore_wait(barrier, 127)
        for copy in borders:
            copy.start()

    bucket(part, dest, ca, cb, send, scell, oh, pos_s, srt, csrt, acc, stv, sts, sem, other, turn, ship, ready, open_links)
    recv[me] = send[me]
    rcell[me] = scell[me]

    def bytes_of(n, src, dst, s_sem, r_sem):
        return pltpu.make_async_remote_copy(
            src_ref=src.at[pl.ds(0, n)],
            dst_ref=dst.at[pl.ds(0, n)],
            send_sem=s_sem,
            recv_sem=r_sem,
            device_id=other(1),
            device_id_type=LOGICAL,
        )

    def arrived(group, n):
        bytes_of(n, send, recv, ss.at[0], ra.at[group]).wait_recv()
        bytes_of(n, scell, rcell, ss.at[1], rb.at[group]).wait_recv()

    for copy in borders:
        copy.wait_recv()
    masks = [(gx > 0).astype(F32), (gx < 3).astype(F32), (col > 0).astype(F32), (col < 31).astype(F32)]
    setup(vel, halo, fh, fl, tab, masks)
    last = 128 // U - 1

    def step(i, k):
        @pl.when(i < last)
        def _full():
            arrived(i, U)

        @pl.when(i == last)
        def _short():
            arrived(last, U - 1)

        for u in range(U):
            k = turn(k)
            s = me - k
            s = jnp.where(s < 0, s + 128, s)
            cell = rcell[s]
            out[:, pl.ds(pl.multiple_of(s * 256, 256), 256)] = interp(recv[s], cell, fh, fl, tab)
            cout[s] = cell.astype(I32)
        return k

    lax.fori_loop(0, 128 // U, step, 0)
    bytes_of(127, send, recv, ss.at[0], ra.at[0]).wait_send()
    bytes_of(127, scell, rcell, ss.at[1], rb.at[0]).wait_send()
    bytes_of(8, halo, halo, ss.at[2], rh.at[0]).wait_send()


def shards(particles, dest_key, cell_a, cell_b, velocity):
    vmem = pl.BlockSpec(memory_space=pltpu.VMEM)
    binned, cells = pl.pallas_call(
        fused,
        out_shape=(jax.ShapeDtypeStruct((8, 32768), F32), jax.ShapeDtypeStruct((128, 1, 256), I32)),
        in_specs=[pl.BlockSpec(memory_space=pl.ANY)] * 5,
        out_specs=[vmem] * 2,
        scratch_shapes=[
            pltpu.VMEM((2, 256, 128), F32),
            pltpu.VMEM((8, 8192), F32),
            pltpu.VMEM((64, 128), I32),
            pltpu.VMEM((64, 128), I32),
            pltpu.VMEM((64, 128), I32),
            pltpu.VMEM((128, 8, 256), F32),
            pltpu.VMEM((128, 1, 256), F32),
            pltpu.VMEM((128, 8, 256), F32),
            pltpu.VMEM((128, 1, 256), F32),
            pltpu.VMEM((4, 2, 256), F32),
            pltpu.VMEM((8, 2, 256), F32),
            pltpu.VMEM((272, 256), BF),
            pltpu.VMEM((272, 256), BF),
            pltpu.VMEM((2, 8, 128), F32),
            pltpu.VMEM((32, 128, 256), BF),
            pltpu.VMEM((32, 2, 256), F32),
            pltpu.VMEM((67, 8, 128), F32),
            pltpu.VMEM((67, 8, 128), F32),
            pltpu.VMEM((576, 256), F32),
            pltpu.VMEM((8, 128), I32),
            pltpu.SMEM((8, 128), I32),
            pltpu.SemaphoreType.DMA,
            pltpu.SemaphoreType.DMA((5,)),
            pltpu.SemaphoreType.DMA((3,)),
            pltpu.SemaphoreType.DMA((128 // U,)),
            pltpu.SemaphoreType.DMA((128 // U,)),
            pltpu.SemaphoreType.DMA((8,)),
        ],
        compiler_params=pltpu.CompilerParams(collective_id=0, has_side_effects=True),
        name="rebin",
    )(velocity, particles, dest_key.reshape(64, 128), cell_a.reshape(64, 128), cell_b.reshape(64, 128))
    return binned, cells.reshape(-1)


def solution(mesh):
    in_specs = (P(None, AXES), P(AXES), P(AXES), P(AXES), P(None, "gx", ("gy", "gz")))
    return jax.shard_map(
        shards, mesh=mesh, in_specs=in_specs, out_specs=(P(None, AXES), P(AXES)), check_vma=False
    )
```

```python
import jax
import jax.numpy as jnp
from jax import lax
from jax.experimental import pallas as pl
from jax.experimental.pallas import tpu as pltpu
from jax.sharding import PartitionSpec as P

BF = jnp.bfloat16
F32 = jnp.float32
I32 = jnp.int32
NT = (((1,), (1,)), ((), ()))
AXES = ("gx", "gy", "gz")
LOGICAL = pl.DeviceIdType.LOGICAL
SIDES = ((1, 1, 0), (0, -1, 0), (3, 0, 1), (2, 0, -1), (1, 1, 1), (1, 1, -1), (0, -1, 1), (0, -1, -1))


def dotf(a, b):
    return jnp.dot(a, b, preferred_element_type=F32)


PB=16
UB=16
XB=16
U=16
STRIDE=27

def row256(ref, j):
    r = ref[pl.ds(2*j,2),:]
    return jnp.concatenate([r[0:1],r[1:2]],axis=1)

def bucket(part, dest, ca, cb, out, cells, oh, pos_s, srt, csrt, acc, stv, sts, sem, target, turn, ship, ready, open_links):
    nb=32
    one=jnp.ones((),BF); zero=jnp.zeros((),BF)
    iod=lax.broadcasted_iota(I32,(128,256),0).astype(F32).astype(BF)
    def onehot(j,S):
        d=row256(dest,j).astype(F32).astype(BF)
        o=jnp.where(iod==jnp.broadcast_to(d,(128,256)),one,zero)
        oh[j]=o
        return S+o
    S=lax.fori_loop(0,nb,onehot,jnp.zeros((128,256),BF),unroll=4)
    ones=jnp.ones((256,256),BF)
    tot=dotf(S,ones)
    low=(lax.broadcasted_iota(I32,(128,128),0)>lax.broadcasted_iota(I32,(128,128),1)).astype(F32).astype(BF)
    start=dotf(low,tot.astype(BF))
    diag=lax.broadcasted_iota(I32,(128,128),0)==lax.broadcasted_iota(I32,(128,128),1)
    srow=jnp.sum(jnp.where(diag,start[:,:128],0.),axis=0,keepdims=True)
    trow=jnp.sum(jnp.where(diag,tot[:,:128],0.),axis=0,keepdims=True)
    tile=jnp.floor(srow*(1/128))
    sh=srow-128.*tile
    stv[0:1,:]=tile.astype(I32)
    stv[1:2,:]=jnp.where(sh==0.,0.,128.-sh).astype(I32)
    stv[2:3,:]=(128.-sh).astype(I32)
    stv[3:4,:]=trow.astype(I32)
    cp=pltpu.make_async_copy(stv,sts,sem)
    cp.start()
    up=(lax.broadcasted_iota(I32,(256,256),0)<lax.broadcasted_iota(I32,(256,256),1)).astype(F32).astype(BF)
    upones=jnp.concatenate([up,ones],axis=0)
    lane=lax.broadcasted_iota(I32,(128,256),1).astype(F32)
    C0=jnp.floor((start+255.-lane)*(1/256)).astype(BF)
    def ranks(jj,C):
        for u in range(PB):
            j=jj*PB+u
            o=oh[j]
            x=dotf(jnp.concatenate([o,C],axis=1),upones)
            pos=jnp.sum(o.astype(F32)*x,axis=0,keepdims=True)
            hi=jnp.floor(pos*(1/256))
            pos_s[j,0:1,:]=hi
            pos_s[j,1:2,:]=pos-256.*hi
            C=C+o
        return C
    lax.fori_loop(0,nb//PB,ranks,C0)
    acc[...]=jnp.zeros_like(acc)
    ready()
    iol=lax.broadcasted_iota(I32,(256,256),0).astype(F32).astype(BF)
    s16=lax.broadcasted_iota(I32,(16,256),0)
    half=(s16//8).astype(F32).astype(BF)
    i32_=lax.broadcasted_iota(I32,(32,256),0).astype(F32).astype(BF)
    def place(jj,_):
        As=[];Ls=[]
        for u in range(UB):
            j=jj*UB+u
            hi=pos_s[j,0:1,:].astype(BF); lo=pos_s[j,1:2,:].astype(BF)
            lot=jnp.where(iol==jnp.broadcast_to(lo,(256,256)),one,zero)
            v=part[:,pl.ds(pl.multiple_of(j*256,256),256)]
            vh=v.astype(BF).astype(F32); vl=v-vh
            vh2=jnp.concatenate([vh,vh],axis=0).astype(BF)
            vl2=jnp.concatenate([vl,vl],axis=0).astype(BF)
            h16=jnp.broadcast_to(hi,(16,256))-half
            hs=[];ls=[]
            for k in range(16):
                m=h16==float(2*k)
                hs.append(jnp.where(m,vh2,zero)); ls.append(jnp.where(m,vl2,zero))
            m32=i32_==jnp.broadcast_to(hi,(32,256))
            a=row256(ca,j).astype(F32).astype(BF); b=row256(cb,j).astype(F32).astype(BF)
            As.append(jnp.concatenate(hs+ls+[jnp.where(m32,jnp.broadcast_to(a,(32,256)),zero),jnp.where(m32,jnp.broadcast_to(b,(32,256)),zero)],axis=0))
            Ls.append(lot)
        acc[...]+=lax.dot_general(jnp.concatenate(As,axis=1),jnp.concatenate(Ls,axis=1),NT,preferred_element_type=F32)
        return _
    lax.fori_loop(0,nb//UB,place,0)
    for h in range(32):
        x=acc[h*8:(h+1)*8]+acc[256+h*8:256+(h+1)*8]
        srt[2*h]=x[:,:128]; srt[2*h+1]=x[:,128:]
    cc=acc[512:544]*128.+acc[544:576]
    for t in range(64):
        r=cc[t//2:t//2+1,(t%2)*128:(t%2)*128+128]
        for i in range(3):
            if t-i>=0: csrt[t-i,i:i+1,:]=r
    cp.wait()
    lane=lax.broadcasted_iota(I32,(8,128),1)
    def expand(k):
        d=target(k)
        t=jnp.clip(sts[0,d],0,64); rot=sts[1,d]; thr=sts[2,d]; n=sts[3,d]
        rs=[pltpu.roll(srt[t+i],rot,1) for i in range(3)]
        c=pltpu.roll(csrt[t],rot,1)
        keep=lane<thr
        c1=jnp.where(keep[0:2],c[0:2],c[1:3])
        for i in range(2):
            live=lane<n-128*i
            out[d,:,128*i:128*(i+1)]=jnp.where(live,jnp.where(keep,rs[i],rs[i+1]),0.)
            cells[d,:,128*i:128*(i+1)]=jnp.where(live[0:1],c1[i:i+1],-1.)
    def back(k):
        k=k-STRIDE*XB%128
        return jnp.where(k<0,k+128,k)
    def deliver(i,k):
        old=k
        for u in range(XB):
            k=turn(k)
            expand(k)
        @pl.when(i>0)
        def _():
            ship(i-1,back(old),XB)
        return k
    open_links()
    k=lax.fori_loop(0,128//XB,deliver,0)
    ship(128//XB-1,back(k),XB-1)

def split(x):
    h=x.astype(BF); return h,(x-h.astype(F32)).astype(BF)
def weights(t):
    return 0.5*t*(t-1.), 1.-t*t, 0.5*t*(t+1.)
def setup(vel, halo, fh, fl, tab, masks):
    mu,md,ml,mr=masks
    lane=lax.broadcasted_iota(I32,(1,128),1)
    z8=jnp.zeros((8,256),F32)
    for c in range(2):
        ft=jnp.transpose(vel[c])
        lrow=halo[2][c:c+1,:]*ml
        rrow=halo[3][c:c+1,:]*mr
        e=jnp.concatenate([lrow,ft,rrow,jnp.zeros((6,256),F32)],axis=0)
        h,l=split(e)
        fh[c*136:(c+1)*136]=h; fl[c*136:(c+1)*136]=l
        rows=[]
        for (mid,lc,rc,m) in ((0,4,5,mu),(1,6,7,md)):
            r=halo[mid][c:c+1,:128]*m
            le=halo[lc][c:c+1,:128]*(m*ml); re=halo[rc][c:c+1,:128]*(m*mr)
            rows.append(jnp.where(lane==0,pltpu.roll(le,1,1),pltpu.roll(r,1,1)))
            rows.append(r)
            rows.append(jnp.where(lane==127,pltpu.roll(re,127,1),pltpu.roll(r,127,1)))
        tab[c]=jnp.concatenate(rows+[jnp.zeros((2,128),F32)],axis=0)
def cellparts(cell):
    cm=jnp.maximum(cell,0.)
    a=jnp.floor(cm*(1/128)); b=cm-128.*a
    return a,b
def pick(rows, bits):
    level=list(rows)
    for m in bits:
        level=[jnp.where(m,level[2*k+1],level[2*k]) for k in range(len(level)//2)]
    return level[0]
def interp(v, cell, fh, fl, tab):
    n=v.shape[1]
    zero=jnp.zeros((),BF)
    f=v[0:1]; g=v[1:2]
    live=cell>=0.
    a,b=cellparts(cell)
    wf=weights(f); wg=weights(g)
    ga=jnp.floor((a-1.)*(1/16)); oa=(a-1.)-16.*ga
    gab=jnp.broadcast_to(ga.astype(BF),(16,n))
    d=lax.broadcasted_iota(I32,(16,n),0).astype(F32).astype(BF)-jnp.broadcast_to(oa.astype(BF),(16,n))
    hl=[split(w) for w in wf]
    m0=d==0;m1=d==1;m2=d==2;q1=d==-15;q2=d==-14
    pats=[]
    for i in range(2):
        w=[jnp.broadcast_to(x[i],(16,n)) for x in hl]
        pats.append((jnp.where(m0,w[0],jnp.where(m1,w[1],jnp.where(m2,w[2],zero))),
                     jnp.where(q1,w[1],jnp.where(q2,w[2],zero))))
    ms=[gab==float(G) for G in range(-1,16)]
    W=[jnp.concatenate([jnp.where(ms[G+1],pa,jnp.where(ms[G],pb,zero)) for G in range(16)],axis=0) for pa,pb in pats]
    H=fh[...]; L=fl[...]
    R=dotf(H,W[0])+dotf(L,W[0])+dotf(H,W[1])
    gb=jnp.floor(b*(1/8)); ob=b-8.*gb
    s8=lax.broadcasted_iota(I32,(8,n),0).astype(F32)
    d8=s8-ob
    pa=jnp.where(d8==0,wg[0],jnp.where(d8==1,wg[1],jnp.where(d8==2,wg[2],0.)))
    pb=jnp.where(d8==-7,wg[1],jnp.where(d8==-6,wg[2],0.))
    gi=jnp.broadcast_to(gb,(8,n)).astype(I32)
    bits=[(gi&(1<<k))!=0 for k in range(4)]
    accs=[]
    for c in range(2):
        rows=[R[c*136+8*G:c*136+8*G+8] for G in range(17)]
        accs.append((pick(rows[:16],bits),pick(rows[1:],bits)))
    si=lax.broadcasted_iota(I32,(8,n),0)
    wj=jnp.where((si==0)|(si==3),wg[0],jnp.where((si==1)|(si==4),wg[1],wg[2]))
    up=jnp.where(a==0.,wf[0],0.); dn=jnp.where(a==255.,wf[2],0.)
    Pm=jnp.where(si<3,up,jnp.where(si<6,dn,0.))*wj
    bi=jnp.broadcast_to(b.astype(I32),(8,n))
    out=v
    for c in range(2):
        T=tab[c]
        corr=jnp.concatenate([jnp.take_along_axis(T,bi[:,128*i:128*(i+1)],axis=1) for i in range(n//128)],axis=1)
        sp=jnp.sum(pa*accs[c][0]+pb*accs[c][1]+Pm*corr,axis=0,keepdims=True)
        disp=jnp.where(live,0.5*sp,0.)
        out=out+jnp.where(si==2+c,disp,0.)
    return out


def fused(vel_in, part_in, dest_in, ca_in, cb_in, out, cout, vel, part, dest, ca, cb, send, scell, recv, rcell, edges, halo,
          fh, fl, tab, oh, pos_s, srt, csrt, acc, stv, sts, sem, ins, ss, ra, rb, rh):
    loads = [
        pltpu.make_async_copy(src, dst, ins.at[i])
        for i, (src, dst) in enumerate(((dest_in, dest), (vel_in, vel), (ca_in, ca), (cb_in, cb), (part_in, part)))
    ]
    for load in loads:
        load.start()
    gx = lax.axis_index("gx")
    col = lax.axis_index("gy") * 2 + lax.axis_index("gz")
    me = gx * 32 + col
    barrier = pltpu.get_barrier_semaphore()

    def wrap(p):
        return jnp.where(p >= 128, p - 128, p)

    def other(k):
        return wrap(me + k)

    def turn(k):
        return wrap(k + STRIDE)

    def greet(k, _):
        pl.semaphore_signal(barrier, inc=1, device_id=other(k), device_id_type=LOGICAL)
        return _

    lax.fori_loop(1, 128, greet, 0)
    loads[0].wait()
    loads[1].wait()
    for c in range(2):
        zeros = jnp.zeros((1, 128), F32)
        edges[0, c : c + 1, :] = jnp.concatenate([vel[c, 0:1, :], zeros], axis=1)
        edges[1, c : c + 1, :] = jnp.concatenate([vel[c, 255:256, :], zeros], axis=1)
        turned = jnp.transpose(vel[c])
        edges[2, c : c + 1, :] = turned[0:1]
        edges[3, c : c + 1, :] = turned[127:128]

    def neighbour(da, db):
        return lax.rem(gx + da + 4, 4) * 32 + lax.rem(col + db + 32, 32)

    borders = []
    for slot, (edge, da, db) in enumerate(SIDES):
        borders.append(
            pltpu.make_async_remote_copy(
                src_ref=edges.at[edge],
                dst_ref=halo.at[slot],
                send_sem=ss.at[2],
                recv_sem=rh.at[slot],
                device_id=neighbour(da, db),
                device_id_type=LOGICAL,
            )
        )

    def ready():
        for load in loads[2:]:
            load.wait()

    def ship(group, k, count):
        for u in range(count):
            k = turn(k)
            p = other(k)
            for src, dst, lane_sem, done in ((send, recv, ss.at[0], ra), (scell, rcell, ss.at[1], rb)):
                pltpu.make_async_remote_copy(
                    src_ref=src.at[p],
                    dst_ref=dst.at[me],
                    send_sem=lane_sem,
                    recv_sem=done.at[group],
                    device_id=p,
                    device_id_type=LOGICAL,
                ).start()

    def open_links():
        pl.semaphore_wait(barrier, 127)
        for copy in borders:
            copy.start()

    bucket(part, dest, ca, cb, send, scell, oh, pos_s, srt, csrt, acc, stv, sts, sem, other, turn, ship, ready, open_links)
    recv[me] = send[me]
    rcell[me] = scell[me]

    def bytes_of(n, src, dst, s_sem, r_sem):
        return pltpu.make_async_remote_copy(
            src_ref=src.at[pl.ds(0, n)],
            dst_ref=dst.at[pl.ds(0, n)],
            send_sem=s_sem,
            recv_sem=r_sem,
            device_id=other(1),
            device_id_type=LOGICAL,
        )

    def arrived(group, n):
        bytes_of(n, send, recv, ss.at[0], ra.at[group]).wait_recv()
        bytes_of(n, scell, rcell, ss.at[1], rb.at[group]).wait_recv()

    for copy in borders:
        copy.wait_recv()
    masks = [(gx > 0).astype(F32), (gx < 3).astype(F32), (col > 0).astype(F32), (col < 31).astype(F32)]
    setup(vel, halo, fh, fl, tab, masks)
    last = 128 // U - 1
    per = U // XB

    def step(i, k):
        @pl.when(i < last)
        def _full():
            for q in range(per):
                arrived(i * per + q, XB)

        @pl.when(i == last)
        def _short():
            for q in range(per):
                arrived(last * per + q, XB - (q == per - 1))

        for u in range(U):
            k = turn(k)
            s = me - k
            s = jnp.where(s < 0, s + 128, s)
            cell = rcell[s]
            out[:, pl.ds(pl.multiple_of(s * 256, 256), 256)] = interp(recv[s], cell, fh, fl, tab)
            cout[s] = cell.astype(I32)
        return k

    lax.fori_loop(0, 128 // U, step, 0)
    bytes_of(127, send, recv, ss.at[0], ra.at[0]).wait_send()
    bytes_of(127, scell, rcell, ss.at[1], rb.at[0]).wait_send()
    bytes_of(8, halo, halo, ss.at[2], rh.at[0]).wait_send()


def put_out(a_ref, b_ref, out, cout, sems):
    copies = [pltpu.make_async_copy(a_ref, out, sems.at[0]), pltpu.make_async_copy(b_ref, cout, sems.at[1])]
    for copy in copies:
        copy.start()
    for copy in copies:
        copy.wait()


def settle(binned, cells):
    binned, cells = pl.pallas_call(
        put_out,
        out_shape=(jax.ShapeDtypeStruct(binned.shape, F32), jax.ShapeDtypeStruct(cells.shape, I32)),
        in_specs=[pl.BlockSpec(memory_space=pltpu.VMEM)] * 2,
        out_specs=[pl.BlockSpec(memory_space=pl.ANY)] * 2,
        scratch_shapes=[pltpu.SemaphoreType.DMA((2,))],
        name="settle",
    )(pltpu.with_memory_space_constraint(binned, pltpu.VMEM), pltpu.with_memory_space_constraint(cells, pltpu.VMEM))
    return binned, cells.reshape(-1)


def shards(particles, dest_key, cell_a, cell_b, velocity):
    vmem = pl.BlockSpec(memory_space=pltpu.VMEM)
    binned, cells = pl.pallas_call(
        fused,
        out_shape=(pltpu.VMEM((8, 32768), F32), pltpu.VMEM((128, 1, 256), I32)),
        in_specs=[pl.BlockSpec(memory_space=pl.ANY)] * 5,
        out_specs=[vmem] * 2,
        scratch_shapes=[
            pltpu.VMEM((2, 256, 128), F32),
            pltpu.VMEM((8, 8192), F32),
            pltpu.VMEM((64, 128), I32),
            pltpu.VMEM((64, 128), I32),
            pltpu.VMEM((64, 128), I32),
            pltpu.VMEM((128, 8, 256), F32),
            pltpu.VMEM((128, 1, 256), F32),
            pltpu.VMEM((128, 8, 256), F32),
            pltpu.VMEM((128, 1, 256), F32),
            pltpu.VMEM((4, 2, 256), F32),
            pltpu.VMEM((8, 2, 256), F32),
            pltpu.VMEM((272, 256), BF),
            pltpu.VMEM((272, 256), BF),
            pltpu.VMEM((2, 8, 128), F32),
            pltpu.VMEM((32, 128, 256), BF),
            pltpu.VMEM((32, 2, 256), F32),
            pltpu.VMEM((67, 8, 128), F32),
            pltpu.VMEM((67, 8, 128), F32),
            pltpu.VMEM((576, 256), F32),
            pltpu.VMEM((8, 128), I32),
            pltpu.SMEM((8, 128), I32),
            pltpu.SemaphoreType.DMA,
            pltpu.SemaphoreType.DMA((5,)),
            pltpu.SemaphoreType.DMA((3,)),
            pltpu.SemaphoreType.DMA((128 // XB,)),
            pltpu.SemaphoreType.DMA((128 // XB,)),
            pltpu.SemaphoreType.DMA((8,)),
        ],
        compiler_params=pltpu.CompilerParams(collective_id=0, has_side_effects=True),
        name="rebin",
    )(velocity, particles, dest_key.reshape(64, 128), cell_a.reshape(64, 128), cell_b.reshape(64, 128))
    return settle(binned, cells)


def solution(mesh):
    in_specs = (P(None, AXES), P(AXES), P(AXES), P(AXES), P(None, "gx", ("gy", "gz")))
    return jax.shard_map(
        shards, mesh=mesh, in_specs=in_specs, out_specs=(P(None, AXES), P(AXES)), check_vma=False
    )
```

```python
import jax
import jax.numpy as jnp
from jax import lax
from jax.experimental import pallas as pl
from jax.experimental.pallas import tpu as pltpu
from jax.sharding import PartitionSpec as P

BF = jnp.bfloat16
F32 = jnp.float32
I32 = jnp.int32
NT = (((1,), (1,)), ((), ()))
AXES = ("gx", "gy", "gz")
LOGICAL = pl.DeviceIdType.LOGICAL
SIDES = ((1, 1, 0), (0, -1, 0), (3, 0, 1), (2, 0, -1), (1, 1, 1), (1, 1, -1), (0, -1, 1), (0, -1, -1))


def dotf(a, b):
    return jnp.dot(a, b, preferred_element_type=F32)


PB=16
UB=16
U=16
STEPS=((4,1),(2,2))
SB=8
TURN=tuple(27*u%128 for u in range(U))
STEP=27*SB%128

def row256(ref, j):
    r = ref[pl.ds(2*j,2),:]
    return jnp.concatenate([r[0:1],r[1:2]],axis=1)

def bucket(part, dest, ca, cb, out, cells, oh, pos_s, srt, csrt, acc, stv, sts, sem, peer, ship, ready, open_links):
    nb=32
    one=jnp.ones((),BF); zero=jnp.zeros((),BF)
    iod=lax.broadcasted_iota(I32,(128,256),0).astype(F32).astype(BF)
    def onehot(j,S):
        d=row256(dest,j).astype(F32).astype(BF)
        o=jnp.where(iod==jnp.broadcast_to(d,(128,256)),one,zero)
        oh[j]=o
        return S+o
    S=lax.fori_loop(0,nb,onehot,jnp.zeros((128,256),BF),unroll=4)
    ones=jnp.ones((256,256),BF)
    tot=dotf(S,ones)
    low=(lax.broadcasted_iota(I32,(128,128),0)>lax.broadcasted_iota(I32,(128,128),1)).astype(F32).astype(BF)
    start=dotf(low,tot.astype(BF))
    diag=lax.broadcasted_iota(I32,(128,128),0)==lax.broadcasted_iota(I32,(128,128),1)
    srow=jnp.sum(jnp.where(diag,start[:,:128],0.),axis=0,keepdims=True)
    trow=jnp.sum(jnp.where(diag,tot[:,:128],0.),axis=0,keepdims=True)
    tile=jnp.floor(srow*(1/128))
    sh=srow-128.*tile
    stv[0:1,:]=(tile+128.*(128.-sh)+32768.*trow).astype(I32)
    cp=pltpu.make_async_copy(stv,sts,sem)
    cp.start()
    up=(lax.broadcasted_iota(I32,(256,256),0)<lax.broadcasted_iota(I32,(256,256),1)).astype(F32).astype(BF)
    first=lax.broadcasted_iota(I32,(256,256),1)==0
    up=jnp.where(first,1.,up.astype(F32)).astype(BF)
    lane=lax.broadcasted_iota(I32,(128,256),1)
    def ranks(jj,base):
        for u in range(PB):
            j=jj*PB+u
            o=oh[j]
            x=dotf(o,up)
            b2=jnp.concatenate([base,base],axis=1)
            pos=jnp.sum(o.astype(F32)*(jnp.where(lane==0,0.,x)+b2),axis=0,keepdims=True)
            hi=jnp.floor(pos*(1/256))
            pos_s[j,0:1,:]=hi
            pos_s[j,1:2,:]=pos-256.*hi
            base=base+jnp.broadcast_to(x[:,0:1],(128,128))
        return base
    lax.fori_loop(0,nb//PB,ranks,start[:,:128])
    acc[...]=jnp.zeros_like(acc)
    ready()
    iol=lax.broadcasted_iota(I32,(256,256),0).astype(F32).astype(BF)
    s16=lax.broadcasted_iota(I32,(16,256),0)
    half=(s16//8).astype(F32).astype(BF)
    i32_=lax.broadcasted_iota(I32,(32,256),0).astype(F32).astype(BF)
    def place(jj,_):
        As=[];Ls=[]
        for u in range(UB):
            j=jj*UB+u
            hi=pos_s[j,0:1,:].astype(BF); lo=pos_s[j,1:2,:].astype(BF)
            lot=jnp.where(iol==jnp.broadcast_to(lo,(256,256)),one,zero)
            v=part[:,pl.ds(pl.multiple_of(j*256,256),256)]
            vh=v.astype(BF).astype(F32); vl=v-vh
            vh2=jnp.concatenate([vh,vh],axis=0).astype(BF)
            vl2=jnp.concatenate([vl,vl],axis=0).astype(BF)
            h16=jnp.broadcast_to(hi,(16,256))-half
            hs=[];ls=[]
            for k in range(16):
                m=h16==float(2*k)
                hs.append(jnp.where(m,vh2,zero)); ls.append(jnp.where(m,vl2,zero))
            m32=i32_==jnp.broadcast_to(hi,(32,256))
            a=row256(ca,j).astype(F32).astype(BF); b=row256(cb,j).astype(F32).astype(BF)
            As.append(jnp.concatenate(hs+ls+[jnp.where(m32,jnp.broadcast_to(a,(32,256)),zero),jnp.where(m32,jnp.broadcast_to(b,(32,256)),zero)],axis=0))
            Ls.append(lot)
        acc[...]+=lax.dot_general(jnp.concatenate(As,axis=1),jnp.concatenate(Ls,axis=1),NT,preferred_element_type=F32)
        return _
    lax.fori_loop(0,nb//UB,place,0)
    for h in range(32):
        x=acc[h*8:(h+1)*8]+acc[256+h*8:256+(h+1)*8]
        srt[2*h]=x[:,:128]; srt[2*h+1]=x[:,128:]
    cc=acc[512:544]*128.+acc[544:576]
    for t in range(64):
        r=cc[t//2:t//2+1,(t%2)*128:(t%2)*128+128]
        for i in range(3):
            if t-i>=0: csrt[t-i,i:i+1,:]=r
    cp.wait()
    lane=lax.broadcasted_iota(I32,(8,128),1)
    lane2=lane+128
    def expand(d):
        w=sts[0,d]
        t=w&127; rot=(w>>7)&255; n=w>>15
        rs=[pltpu.roll(srt[t+i],rot,1) for i in range(3)]
        c=pltpu.roll(csrt[t],rot,1)
        keep=lane<rot
        c1=jnp.where(keep[0:2],c[0:2],c[1:3])
        for i,at in enumerate((lane,lane2)):
            live=at<n
            out[d,:,128*i:128*(i+1)]=jnp.where(live,jnp.where(keep,rs[i],rs[i+1]),0.)
            cells[d,:,128*i:128*(i+1)]=jnp.where(live[0:1],c1[i:i+1],-1.)
    open_links()
    first=peer(0,0)
    second=wrap(first+STEP)
    for base in (first,second):
        for u in range(SB):
            expand(wrap(base+TURN[u]))
    ship(0,first,1)
    def deliver(m,base):
        now=wrap(base+STEP)
        for u in range(SB):
            expand(wrap(now+TURN[u]))
        ship((m-1)//(U//SB),base,0)
        return now
    last=lax.fori_loop(2,128//SB,deliver,second)
    ship(128//U-1,last,0)

def wrap(p):
    return jnp.where(p >= 128, p - 128, p)

def split(x):
    h=x.astype(BF); return h,(x-h.astype(F32)).astype(BF)
def weights(t):
    return 0.5*t*(t-1.), 1.-t*t, 0.5*t*(t+1.)
def setup(vel, halo, fh, fl, tab, masks):
    mu,md,ml,mr=masks
    lane=lax.broadcasted_iota(I32,(1,128),1)
    z8=jnp.zeros((8,256),F32)
    for c in range(2):
        ft=jnp.transpose(vel[c])
        lrow=halo[2][c:c+1,:]*ml
        rrow=halo[3][c:c+1,:]*mr
        e=jnp.concatenate([lrow,ft,rrow,jnp.zeros((6,256),F32)],axis=0)
        h,l=split(e)
        fh[c*136:(c+1)*136]=h; fl[c*136:(c+1)*136]=l
        rows=[]
        for (mid,lc,rc,m) in ((0,4,5,mu),(1,6,7,md)):
            r=halo[mid][c:c+1,:128]*m
            le=halo[lc][c:c+1,:128]*(m*ml); re=halo[rc][c:c+1,:128]*(m*mr)
            rows.append(jnp.where(lane==0,pltpu.roll(le,1,1),pltpu.roll(r,1,1)))
            rows.append(r)
            rows.append(jnp.where(lane==127,pltpu.roll(re,127,1),pltpu.roll(r,127,1)))
        tab[c]=jnp.concatenate(rows+[jnp.zeros((2,128),F32)],axis=0)
def cellparts(cell):
    cm=jnp.maximum(cell,0.)
    a=jnp.floor(cm*(1/128)); b=cm-128.*a
    return a,b
def pick(rows, bits):
    level=list(rows)
    for m in bits:
        level=[jnp.where(m,level[2*k+1],level[2*k]) for k in range(len(level)//2)]
    return level[0]
def interp(v, cell, fh, fl, tab):
    n=v.shape[1]
    zero=jnp.zeros((),BF)
    f=v[0:1]; g=v[1:2]
    live=cell>=0.
    a,b=cellparts(cell)
    wf=weights(f); wg=weights(g)
    ga=jnp.floor((a-1.)*(1/16)); oa=(a-1.)-16.*ga
    gab=jnp.broadcast_to(ga.astype(BF),(16,n))
    d=lax.broadcasted_iota(I32,(16,n),0).astype(F32).astype(BF)-jnp.broadcast_to(oa.astype(BF),(16,n))
    hl=[split(w) for w in wf]
    m0=d==0;m1=d==1;m2=d==2;q1=d==-15;q2=d==-14
    pats=[]
    for i in range(2):
        w=[jnp.broadcast_to(x[i],(16,n)) for x in hl]
        pats.append((jnp.where(m0,w[0],jnp.where(m1,w[1],jnp.where(m2,w[2],zero))),
                     jnp.where(q1,w[1],jnp.where(q2,w[2],zero))))
    ms=[gab==float(G) for G in range(-1,16)]
    W=[jnp.concatenate([jnp.where(ms[G+1],pa,jnp.where(ms[G],pb,zero)) for G in range(16)],axis=0) for pa,pb in pats]
    H=fh[...]; L=fl[...]
    R=dotf(H,W[0])+dotf(L,W[0])+dotf(H,W[1])
    gb=jnp.floor(b*(1/8)); ob=b-8.*gb
    s8=lax.broadcasted_iota(I32,(8,n),0).astype(F32)
    d8=s8-ob
    pa=jnp.where(d8==0,wg[0],jnp.where(d8==1,wg[1],jnp.where(d8==2,wg[2],0.)))
    pb=jnp.where(d8==-7,wg[1],jnp.where(d8==-6,wg[2],0.))
    gi=jnp.broadcast_to(gb,(8,n)).astype(I32)
    bits=[(gi&(1<<k))!=0 for k in range(4)]
    accs=[]
    for c in range(2):
        rows=[R[c*136+8*G:c*136+8*G+8] for G in range(17)]
        accs.append((pick(rows[:16],bits),pick(rows[1:],bits)))
    si=lax.broadcasted_iota(I32,(8,n),0)
    wj=jnp.where((si==0)|(si==3),wg[0],jnp.where((si==1)|(si==4),wg[1],wg[2]))
    up=jnp.where(a==0.,wf[0],0.); dn=jnp.where(a==255.,wf[2],0.)
    Pm=jnp.where(si<3,up,jnp.where(si<6,dn,0.))*wj
    bi=jnp.broadcast_to(b.astype(I32),(8,n))
    out=v
    for c in range(2):
        T=tab[c]
        corr=jnp.concatenate([jnp.take_along_axis(T,bi[:,128*i:128*(i+1)],axis=1) for i in range(n//128)],axis=1)
        sp=jnp.sum(pa*accs[c][0]+pb*accs[c][1]+Pm*corr,axis=0,keepdims=True)
        disp=jnp.where(live,0.5*sp,0.)
        out=out+jnp.where(si==2+c,disp,0.)
    return out


def fused(vel_in, part_in, dest_in, ca_in, cb_in, out, cout, vel, part, dest, ca, cb, send, scell, recv, rcell, edges, halo,
          fh, fl, tab, oh, pos_s, srt, csrt, acc, stv, sts, sem, ins, ss, ra, rb, rh):
    loads = [
        pltpu.make_async_copy(src, dst, ins.at[i])
        for i, (src, dst) in enumerate(((dest_in, dest), (vel_in, vel), (ca_in, ca), (cb_in, cb), (part_in, part)))
    ]
    for load in loads:
        load.start()
    gx = lax.axis_index("gx")
    col = lax.axis_index("gy") * 2 + lax.axis_index("gz")
    me = gx * 32 + col
    barrier = pltpu.get_barrier_semaphore()

    def other(k):
        return wrap(me + k)

    def peer(i, u):
        return wrap(other(lax.rem(i * (TURN[1] * U), 128)) + TURN[u])

    def origin(i, u):
        s = me - lax.rem(i * (TURN[1] * U), 128)
        s = jnp.where(s < 0, s + 128, s) - TURN[u]
        return jnp.where(s < 0, s + 128, s)

    def greet(k, _):
        pl.semaphore_signal(barrier, inc=1, device_id=other(k), device_id_type=LOGICAL)
        return _

    lax.fori_loop(1, 128, greet, 0)
    loads[0].wait()
    loads[1].wait()
    for c in range(2):
        zeros = jnp.zeros((1, 128), F32)
        edges[0, c : c + 1, :] = jnp.concatenate([vel[c, 0:1, :], zeros], axis=1)
        edges[1, c : c + 1, :] = jnp.concatenate([vel[c, 255:256, :], zeros], axis=1)
        turned = jnp.transpose(vel[c])
        edges[2, c : c + 1, :] = turned[0:1]
        edges[3, c : c + 1, :] = turned[127:128]

    def neighbour(da, db):
        return lax.rem(gx + da + 4, 4) * 32 + lax.rem(col + db + 32, 32)

    borders = []
    for slot, (edge, da, db) in enumerate(SIDES):
        borders.append(
            pltpu.make_async_remote_copy(
                src_ref=edges.at[edge],
                dst_ref=halo.at[slot],
                send_sem=ss.at[2],
                recv_sem=rh.at[slot],
                device_id=neighbour(da, db),
                device_id_type=LOGICAL,
            )
        )

    def ready():
        for load in loads[2:]:
            load.wait()

    def ship(group, base, at):
        for u in range(at, SB):
            p = wrap(base + TURN[u])
            for src, dst, lane_sem, done in ((send, recv, ss.at[0], ra), (scell, rcell, ss.at[1], rb)):
                pltpu.make_async_remote_copy(
                    src_ref=src.at[p],
                    dst_ref=dst.at[me],
                    send_sem=lane_sem,
                    recv_sem=done.at[group],
                    device_id=p,
                    device_id_type=LOGICAL,
                ).start()

    def open_links():
        pl.semaphore_wait(barrier, 127)
        for copy in borders:
            copy.start()

    bucket(part, dest, ca, cb, send, scell, oh, pos_s, srt, csrt, acc, stv, sts, sem, peer, ship, ready, open_links)
    recv[me] = send[me]
    rcell[me] = scell[me]

    def bytes_of(n, src, dst, s_sem, r_sem):
        return pltpu.make_async_remote_copy(
            src_ref=src.at[pl.ds(0, n)],
            dst_ref=dst.at[pl.ds(0, n)],
            send_sem=s_sem,
            recv_sem=r_sem,
            device_id=other(1),
            device_id_type=LOGICAL,
        )

    def arrived(group, n):
        bytes_of(n, send, recv, ss.at[0], ra.at[group]).wait_recv()
        bytes_of(n, scell, rcell, ss.at[1], rb.at[group]).wait_recv()

    for copy in borders:
        copy.wait_recv()
    masks = [(gx > 0).astype(F32), (gx < 3).astype(F32), (col > 0).astype(F32), (col < 31).astype(F32)]
    setup(vel, halo, fh, fl, tab, masks)
    def sources(group, count):
        for q in range(count):

            @pl.when(group + q > 0)
            def _full():
                arrived(group + q, U)

            if q == 0:

                @pl.when(group == 0)
                def _short():
                    arrived(0, U - 1)

        for q in range(count):
            for u in range(U):
                s = origin(group + q, u)
                cell = rcell[s]
                out[:, pl.ds(pl.multiple_of(s * 256, 256), 256)] = interp(recv[s], cell, fh, fl, tab)
                cout[s] = cell.astype(I32)

    done = 0
    for times, count in STEPS:

        def step(i, _, done=done, count=count):
            sources(done + i * count, count)
            return _

        lax.fori_loop(0, times, step, 0)
        done += times * count
    bytes_of(127, send, recv, ss.at[0], ra.at[0]).wait_send()
    bytes_of(127, scell, rcell, ss.at[1], rb.at[0]).wait_send()
    bytes_of(8, halo, halo, ss.at[2], rh.at[0]).wait_send()


def put_out(a_ref, b_ref, out, cout, sems):
    copies = [pltpu.make_async_copy(a_ref, out, sems.at[0]), pltpu.make_async_copy(b_ref, cout, sems.at[1])]
    for copy in copies:
        copy.start()
    for copy in copies:
        copy.wait()


def settle(binned, cells):
    binned, cells = pl.pallas_call(
        put_out,
        out_shape=(jax.ShapeDtypeStruct(binned.shape, F32), jax.ShapeDtypeStruct(cells.shape, I32)),
        in_specs=[pl.BlockSpec(memory_space=pltpu.VMEM)] * 2,
        out_specs=[pl.BlockSpec(memory_space=pl.ANY)] * 2,
        scratch_shapes=[pltpu.SemaphoreType.DMA((2,))],
        name="settle",
    )(pltpu.with_memory_space_constraint(binned, pltpu.VMEM), pltpu.with_memory_space_constraint(cells, pltpu.VMEM))
    return binned, cells.reshape(-1)


def shards(particles, dest_key, cell_a, cell_b, velocity):
    vmem = pl.BlockSpec(memory_space=pltpu.VMEM)
    binned, cells = pl.pallas_call(
        fused,
        out_shape=(pltpu.VMEM((8, 32768), F32), pltpu.VMEM((128, 1, 256), I32)),
        in_specs=[pl.BlockSpec(memory_space=pl.ANY)] * 5,
        out_specs=[vmem] * 2,
        scratch_shapes=[
            pltpu.VMEM((2, 256, 128), F32),
            pltpu.VMEM((8, 8192), F32),
            pltpu.VMEM((64, 128), I32),
            pltpu.VMEM((64, 128), I32),
            pltpu.VMEM((64, 128), I32),
            pltpu.VMEM((128, 8, 256), F32),
            pltpu.VMEM((128, 1, 256), F32),
            pltpu.VMEM((128, 8, 256), F32),
            pltpu.VMEM((128, 1, 256), F32),
            pltpu.VMEM((4, 2, 256), F32),
            pltpu.VMEM((8, 2, 256), F32),
            pltpu.VMEM((272, 256), BF),
            pltpu.VMEM((272, 256), BF),
            pltpu.VMEM((2, 8, 128), F32),
            pltpu.VMEM((32, 128, 256), BF),
            pltpu.VMEM((32, 2, 256), F32),
            pltpu.VMEM((130, 8, 128), F32),
            pltpu.VMEM((130, 8, 128), F32),
            pltpu.VMEM((576, 256), F32),
            pltpu.VMEM((8, 128), I32),
            pltpu.SMEM((8, 128), I32),
            pltpu.SemaphoreType.DMA,
            pltpu.SemaphoreType.DMA((5,)),
            pltpu.SemaphoreType.DMA((3,)),
            pltpu.SemaphoreType.DMA((128 // U,)),
            pltpu.SemaphoreType.DMA((128 // U,)),
            pltpu.SemaphoreType.DMA((8,)),
        ],
        compiler_params=pltpu.CompilerParams(collective_id=0, has_side_effects=True),
        name="rebin",
    )(velocity, particles, dest_key.reshape(64, 128), cell_a.reshape(64, 128), cell_b.reshape(64, 128))
    return settle(binned, cells)


def solution(mesh):
    in_specs = (P(None, AXES), P(AXES), P(AXES), P(AXES), P(None, "gx", ("gy", "gz")))
    return jax.shard_map(
        shards, mesh=mesh, in_specs=in_specs, out_specs=(P(None, AXES), P(AXES)), check_vma=False
    )
```

```python
import jax
import jax.numpy as jnp
from jax import lax
from jax.experimental import pallas as pl
from jax.experimental.pallas import tpu as pltpu
from jax.sharding import PartitionSpec as P

BF = jnp.bfloat16
F32 = jnp.float32
I32 = jnp.int32
NT = (((1,), (1,)), ((), ()))
AXES = ("gx", "gy", "gz")
LOGICAL = pl.DeviceIdType.LOGICAL
SIDES = ((1, 1, 0), (0, -1, 0), (3, 0, 1), (2, 0, -1), (1, 1, 1), (1, 1, -1), (0, -1, 1), (0, -1, -1))


def dotf(a, b):
    return jnp.dot(a, b, preferred_element_type=F32)


PB=32
UB=32
U=16
STEPS=((4,1),(2,2))
SB=8
TURN=tuple(27*u%128 for u in range(U))
STEP=27*SB%128

def row256(ref, j):
    r = ref[pl.ds(2*j,2),:]
    return jnp.concatenate([r[0:1],r[1:2]],axis=1)

def bucket(part, dest, ca, cb, out, cells, oh, pos_s, srt, csrt, acc, stv, sts, sem, peer, ship, ready, open_links):
    nb=32
    one=jnp.ones((),BF); zero=jnp.zeros((),BF)
    iod=lax.broadcasted_iota(I32,(128,256),0).astype(F32).astype(BF)
    def onehot(j,S):
        d=row256(dest,j).astype(F32).astype(BF)
        o=jnp.where(iod==jnp.broadcast_to(d,(128,256)),one,zero)
        oh[j]=o
        return S+o
    S=lax.fori_loop(0,nb,onehot,jnp.zeros((128,256),BF),unroll=4)
    ones=jnp.ones((256,256),BF)
    tot=dotf(S,ones)
    low=(lax.broadcasted_iota(I32,(128,128),0)>lax.broadcasted_iota(I32,(128,128),1)).astype(F32).astype(BF)
    start=dotf(low,tot.astype(BF))
    diag=lax.broadcasted_iota(I32,(128,128),0)==lax.broadcasted_iota(I32,(128,128),1)
    srow=jnp.sum(jnp.where(diag,start[:,:128],0.),axis=0,keepdims=True)
    trow=jnp.sum(jnp.where(diag,tot[:,:128],0.),axis=0,keepdims=True)
    tile=jnp.floor(srow*(1/128))
    sh=srow-128.*tile
    stv[0:1,:]=(tile+128.*(128.-sh)+32768.*trow).astype(I32)
    cp=pltpu.make_async_copy(stv,sts,sem)
    cp.start()
    up=(lax.broadcasted_iota(I32,(256,256),0)<lax.broadcasted_iota(I32,(256,256),1)).astype(F32).astype(BF)
    first=lax.broadcasted_iota(I32,(256,256),1)==0
    up=jnp.where(first,1.,up.astype(F32)).astype(BF)
    lane=lax.broadcasted_iota(I32,(128,256),1)
    def ranks(jj,base):
        for u in range(PB):
            j=jj*PB+u
            o=oh[j]
            x=dotf(o,up)
            b2=jnp.concatenate([base,base],axis=1)
            pos=jnp.sum(o.astype(F32)*(jnp.where(lane==0,0.,x)+b2),axis=0,keepdims=True)
            hi=jnp.floor(pos*(1/256))
            pos_s[j,0:1,:]=hi
            pos_s[j,1:2,:]=pos-256.*hi
            base=base+jnp.broadcast_to(x[:,0:1],(128,128))
        return base
    ranks(0,start[:,:128])
    ready()
    iol=lax.broadcasted_iota(I32,(256,256),0).astype(F32).astype(BF)
    s16=lax.broadcasted_iota(I32,(16,256),0)
    half=(s16//8).astype(F32).astype(BF)
    i32_=lax.broadcasted_iota(I32,(32,256),0).astype(F32).astype(BF)
    def place(jj,_):
        As=[];Ls=[]
        for u in range(UB):
            j=jj*UB+u
            hi=pos_s[j,0:1,:].astype(BF); lo=pos_s[j,1:2,:].astype(BF)
            lot=jnp.where(iol==jnp.broadcast_to(lo,(256,256)),one,zero)
            v=part[:,j*256:(j+1)*256]
            vh=v.astype(BF).astype(F32); vl=v-vh
            vh2=jnp.concatenate([vh,vh],axis=0).astype(BF)
            vl2=jnp.concatenate([vl,vl],axis=0).astype(BF)
            h16=jnp.broadcast_to(hi,(16,256))-half
            hs=[];ls=[]
            for k in range(16):
                m=h16==float(2*k)
                hs.append(jnp.where(m,vh2,zero)); ls.append(jnp.where(m,vl2,zero))
            m32=i32_==jnp.broadcast_to(hi,(32,256))
            a=row256(ca,j).astype(F32).astype(BF); b=row256(cb,j).astype(F32).astype(BF)
            As.append(jnp.concatenate(hs+ls+[jnp.where(m32,jnp.broadcast_to(a,(32,256)),zero),jnp.where(m32,jnp.broadcast_to(b,(32,256)),zero)],axis=0))
            Ls.append(lot)
        acc[...]=lax.dot_general(jnp.concatenate(As,axis=1),jnp.concatenate(Ls,axis=1),NT,preferred_element_type=F32)
        return _
    place(0,0)
    for h in range(32):
        x=acc[h*8:(h+1)*8]+acc[256+h*8:256+(h+1)*8]
        srt[2*h]=x[:,:128]; srt[2*h+1]=x[:,128:]
    cc=acc[512:544]*128.+acc[544:576]
    for t in range(64):
        r=cc[t//2:t//2+1,(t%2)*128:(t%2)*128+128]
        for i in range(3):
            if t-i>=0: csrt[t-i,i:i+1,:]=r
    cp.wait()
    lane=lax.broadcasted_iota(I32,(8,128),1)
    lane2=lane+128
    def expand(d):
        w=sts[0,d]
        t=w&127; rot=(w>>7)&255; n=w>>15
        rs=[pltpu.roll(srt[t+i],rot,1) for i in range(3)]
        c=pltpu.roll(csrt[t],rot,1)
        keep=lane<rot
        c1=jnp.where(keep[0:2],c[0:2],c[1:3])
        for i,at in enumerate((lane,lane2)):
            live=at<n
            out[d,:,128*i:128*(i+1)]=jnp.where(live,jnp.where(keep,rs[i],rs[i+1]),0.)
            cells[d,:,128*i:128*(i+1)]=jnp.where(live[0:1],c1[i:i+1],-1.)
    open_links()
    first=peer(0,0)
    second=wrap(first+STEP)
    for base in (first,second):
        for u in range(SB):
            expand(wrap(base+TURN[u]))
    ship(0,first,1)
    def deliver(m,base):
        now=wrap(base+STEP)
        for u in range(SB):
            expand(wrap(now+TURN[u]))
        ship((m-1)//(U//SB),base,0)
        return now
    last=lax.fori_loop(2,128//SB,deliver,second)
    ship(128//U-1,last,0)

def wrap(p):
    return jnp.where(p >= 128, p - 128, p)

def split(x):
    h=x.astype(BF); return h,(x-h.astype(F32)).astype(BF)
def weights(t):
    return 0.5*t*(t-1.), 1.-t*t, 0.5*t*(t+1.)
def setup(vel, halo, fh, fl, tab, masks):
    mu,md,ml,mr=masks
    lane=lax.broadcasted_iota(I32,(1,128),1)
    z8=jnp.zeros((8,256),F32)
    for c in range(2):
        ft=jnp.transpose(vel[c])
        lrow=halo[2][c:c+1,:]*ml
        rrow=halo[3][c:c+1,:]*mr
        e=jnp.concatenate([lrow,ft,rrow,jnp.zeros((6,256),F32)],axis=0)
        h,l=split(e)
        fh[c*136:(c+1)*136]=h; fl[c*136:(c+1)*136]=l
        rows=[]
        for (mid,lc,rc,m) in ((0,4,5,mu),(1,6,7,md)):
            r=halo[mid][c:c+1,:128]*m
            le=halo[lc][c:c+1,:128]*(m*ml); re=halo[rc][c:c+1,:128]*(m*mr)
            rows.append(jnp.where(lane==0,pltpu.roll(le,1,1),pltpu.roll(r,1,1)))
            rows.append(r)
            rows.append(jnp.where(lane==127,pltpu.roll(re,127,1),pltpu.roll(r,127,1)))
        tab[c]=jnp.concatenate(rows+[jnp.zeros((2,128),F32)],axis=0)
def cellparts(cell):
    cm=jnp.maximum(cell,0.)
    a=jnp.floor(cm*(1/128)); b=cm-128.*a
    return a,b
def pick(rows, bits):
    level=list(rows)
    for m in bits:
        level=[jnp.where(m,level[2*k+1],level[2*k]) for k in range(len(level)//2)]
    return level[0]
def interp(v, cell, fh, fl, tab):
    n=v.shape[1]
    zero=jnp.zeros((),BF)
    f=v[0:1]; g=v[1:2]
    live=cell>=0.
    a,b=cellparts(cell)
    wf=weights(f); wg=weights(g)
    ga=jnp.floor((a-1.)*(1/16)); oa=(a-1.)-16.*ga
    gab=jnp.broadcast_to(ga.astype(BF),(16,n))
    d=lax.broadcasted_iota(I32,(16,n),0).astype(F32).astype(BF)-jnp.broadcast_to(oa.astype(BF),(16,n))
    hl=[split(w) for w in wf]
    m0=d==0;m1=d==1;m2=d==2;q1=d==-15;q2=d==-14
    pats=[]
    for i in range(2):
        w=[jnp.broadcast_to(x[i],(16,n)) for x in hl]
        pats.append((jnp.where(m0,w[0],jnp.where(m1,w[1],jnp.where(m2,w[2],zero))),
                     jnp.where(q1,w[1],jnp.where(q2,w[2],zero))))
    ms=[gab==float(G) for G in range(-1,16)]
    W=[jnp.concatenate([jnp.where(ms[G+1],pa,jnp.where(ms[G],pb,zero)) for G in range(16)],axis=0) for pa,pb in pats]
    H=fh[...]; L=fl[...]
    R=dotf(H,W[0])+dotf(L,W[0])+dotf(H,W[1])
    gb=jnp.floor(b*(1/8)); ob=b-8.*gb
    s8=lax.broadcasted_iota(I32,(8,n),0).astype(F32)
    d8=s8-ob
    pa=jnp.where(d8==0,wg[0],jnp.where(d8==1,wg[1],jnp.where(d8==2,wg[2],0.)))
    pb=jnp.where(d8==-7,wg[1],jnp.where(d8==-6,wg[2],0.))
    gi=jnp.broadcast_to(gb,(8,n)).astype(I32)
    bits=[(gi&(1<<k))!=0 for k in range(4)]
    accs=[]
    for c in range(2):
        rows=[R[c*136+8*G:c*136+8*G+8] for G in range(17)]
        accs.append((pick(rows[:16],bits),pick(rows[1:],bits)))
    si=lax.broadcasted_iota(I32,(8,n),0)
    wj=jnp.where((si==0)|(si==3),wg[0],jnp.where((si==1)|(si==4),wg[1],wg[2]))
    up=jnp.where(a==0.,wf[0],0.); dn=jnp.where(a==255.,wf[2],0.)
    Pm=jnp.where(si<3,up,jnp.where(si<6,dn,0.))*wj
    bi=jnp.broadcast_to(b.astype(I32),(8,n))
    out=v
    for c in range(2):
        T=tab[c]
        corr=jnp.concatenate([jnp.take_along_axis(T,bi[:,128*i:128*(i+1)],axis=1) for i in range(n//128)],axis=1)
        sp=jnp.sum(pa*accs[c][0]+pb*accs[c][1]+Pm*corr,axis=0,keepdims=True)
        disp=jnp.where(live,0.5*sp,0.)
        out=out+jnp.where(si==2+c,disp,0.)
    return out


def fused(vel_in, part_in, dest_in, ca_in, cb_in, out, cout, vel, part, dest, ca, cb, send, scell, recv, rcell, edges, halo,
          fh, fl, tab, oh, pos_s, srt, csrt, acc, stv, sts, sem, ins, ss, ra, rb, rh):
    loads = [
        pltpu.make_async_copy(src, dst, ins.at[i])
        for i, (src, dst) in enumerate(((dest_in, dest), (vel_in, vel), (ca_in, ca), (cb_in, cb), (part_in, part)))
    ]
    for load in loads:
        load.start()
    gx = lax.axis_index("gx")
    col = lax.axis_index("gy") * 2 + lax.axis_index("gz")
    me = gx * 32 + col
    barrier = pltpu.get_barrier_semaphore()

    def other(k):
        return wrap(me + k)

    def peer(i, u):
        return wrap(other(lax.rem(i * (TURN[1] * U), 128)) + TURN[u])

    def origin(i, u):
        s = me - lax.rem(i * (TURN[1] * U), 128)
        s = jnp.where(s < 0, s + 128, s) - TURN[u]
        return jnp.where(s < 0, s + 128, s)

    def greet(k, _):
        pl.semaphore_signal(barrier, inc=1, device_id=other(k), device_id_type=LOGICAL)
        return _

    lax.fori_loop(1, 128, greet, 0)
    loads[0].wait()
    loads[1].wait()
    for c in range(2):
        zeros = jnp.zeros((1, 128), F32)
        edges[0, c : c + 1, :] = jnp.concatenate([vel[c, 0:1, :], zeros], axis=1)
        edges[1, c : c + 1, :] = jnp.concatenate([vel[c, 255:256, :], zeros], axis=1)
        turned = jnp.transpose(vel[c])
        edges[2, c : c + 1, :] = turned[0:1]
        edges[3, c : c + 1, :] = turned[127:128]

    def neighbour(da, db):
        return lax.rem(gx + da + 4, 4) * 32 + lax.rem(col + db + 32, 32)

    borders = []
    for slot, (edge, da, db) in enumerate(SIDES):
        borders.append(
            pltpu.make_async_remote_copy(
                src_ref=edges.at[edge],
                dst_ref=halo.at[slot],
                send_sem=ss.at[2],
                recv_sem=rh.at[slot],
                device_id=neighbour(da, db),
                device_id_type=LOGICAL,
            )
        )

    def ready():
        for load in loads[2:]:
            load.wait()

    def ship(group, base, at):
        for u in range(at, SB):
            p = wrap(base + TURN[u])
            for src, dst, lane_sem, done in ((send, recv, ss.at[0], ra), (scell, rcell, ss.at[1], rb)):
                pltpu.make_async_remote_copy(
                    src_ref=src.at[p],
                    dst_ref=dst.at[me],
                    send_sem=lane_sem,
                    recv_sem=done.at[group],
                    device_id=p,
                    device_id_type=LOGICAL,
                ).start()

    def open_links():
        pl.semaphore_wait(barrier, 127)
        for copy in borders:
            copy.start()

    bucket(part, dest, ca, cb, send, scell, oh, pos_s, srt, csrt, acc, stv, sts, sem, peer, ship, ready, open_links)
    recv[me] = send[me]
    rcell[me] = scell[me]

    def bytes_of(n, src, dst, s_sem, r_sem):
        return pltpu.make_async_remote_copy(
            src_ref=src.at[pl.ds(0, n)],
            dst_ref=dst.at[pl.ds(0, n)],
            send_sem=s_sem,
            recv_sem=r_sem,
            device_id=other(1),
            device_id_type=LOGICAL,
        )

    def arrived(group, n):
        bytes_of(n, send, recv, ss.at[0], ra.at[group]).wait_recv()
        bytes_of(n, scell, rcell, ss.at[1], rb.at[group]).wait_recv()

    for copy in borders:
        copy.wait_recv()
    masks = [(gx > 0).astype(F32), (gx < 3).astype(F32), (col > 0).astype(F32), (col < 31).astype(F32)]
    setup(vel, halo, fh, fl, tab, masks)
    def sources(group, count):
        for q in range(count):

            @pl.when(group + q > 0)
            def _full():
                arrived(group + q, U)

            if q == 0:

                @pl.when(group == 0)
                def _short():
                    arrived(0, U - 1)

        for q in range(count):
            for u in range(U):
                s = origin(group + q, u)
                cell = rcell[s]
                out[:, pl.ds(pl.multiple_of(s * 256, 256), 256)] = interp(recv[s], cell, fh, fl, tab)
                cout[s] = cell.astype(I32)

    done = 0
    for times, count in STEPS:

        def step(i, _, done=done, count=count):
            sources(done + i * count, count)
            return _

        lax.fori_loop(0, times, step, 0)
        done += times * count
    bytes_of(127, send, recv, ss.at[0], ra.at[0]).wait_send()
    bytes_of(127, scell, rcell, ss.at[1], rb.at[0]).wait_send()
    bytes_of(8, halo, halo, ss.at[2], rh.at[0]).wait_send()


def put_out(a_ref, b_ref, out, cout, sems):
    copies = [pltpu.make_async_copy(a_ref, out, sems.at[0]), pltpu.make_async_copy(b_ref, cout, sems.at[1])]
    for copy in copies:
        copy.start()
    for copy in copies:
        copy.wait()


def settle(binned, cells):
    binned, cells = pl.pallas_call(
        put_out,
        out_shape=(jax.ShapeDtypeStruct(binned.shape, F32), jax.ShapeDtypeStruct(cells.shape, I32)),
        in_specs=[pl.BlockSpec(memory_space=pltpu.VMEM)] * 2,
        out_specs=[pl.BlockSpec(memory_space=pl.ANY)] * 2,
        scratch_shapes=[pltpu.SemaphoreType.DMA((2,))],
        name="settle",
    )(pltpu.with_memory_space_constraint(binned, pltpu.VMEM), pltpu.with_memory_space_constraint(cells, pltpu.VMEM))
    return binned, cells.reshape(-1)


def shards(particles, dest_key, cell_a, cell_b, velocity):
    vmem = pl.BlockSpec(memory_space=pltpu.VMEM)
    binned, cells = pl.pallas_call(
        fused,
        out_shape=(pltpu.VMEM((8, 32768), F32), pltpu.VMEM((128, 1, 256), I32)),
        in_specs=[pl.BlockSpec(memory_space=pl.ANY)] * 5,
        out_specs=[vmem] * 2,
        scratch_shapes=[
            pltpu.VMEM((2, 256, 128), F32),
            pltpu.VMEM((8, 8192), F32),
            pltpu.VMEM((64, 128), I32),
            pltpu.VMEM((64, 128), I32),
            pltpu.VMEM((64, 128), I32),
            pltpu.VMEM((128, 8, 256), F32),
            pltpu.VMEM((128, 1, 256), F32),
            pltpu.VMEM((128, 8, 256), F32),
            pltpu.VMEM((128, 1, 256), F32),
            pltpu.VMEM((4, 2, 256), F32),
            pltpu.VMEM((8, 2, 256), F32),
            pltpu.VMEM((272, 256), BF),
            pltpu.VMEM((272, 256), BF),
            pltpu.VMEM((2, 8, 128), F32),
            pltpu.VMEM((32, 128, 256), BF),
            pltpu.VMEM((32, 2, 256), F32),
            pltpu.VMEM((130, 8, 128), F32),
            pltpu.VMEM((130, 8, 128), F32),
            pltpu.VMEM((576, 256), F32),
            pltpu.VMEM((8, 128), I32),
            pltpu.SMEM((8, 128), I32),
            pltpu.SemaphoreType.DMA,
            pltpu.SemaphoreType.DMA((5,)),
            pltpu.SemaphoreType.DMA((3,)),
            pltpu.SemaphoreType.DMA((128 // U,)),
            pltpu.SemaphoreType.DMA((128 // U,)),
            pltpu.SemaphoreType.DMA((8,)),
        ],
        compiler_params=pltpu.CompilerParams(collective_id=0, has_side_effects=True),
        name="rebin",
    )(velocity, particles, dest_key.reshape(64, 128), cell_a.reshape(64, 128), cell_b.reshape(64, 128))
    return settle(binned, cells)


def solution(mesh):
    in_specs = (P(None, AXES), P(AXES), P(AXES), P(AXES), P(None, "gx", ("gy", "gz")))
    return jax.shard_map(
        shards, mesh=mesh, in_specs=in_specs, out_specs=(P(None, AXES), P(AXES)), check_vma=False
    )
```

```python
import jax
import jax.numpy as jnp
from jax import lax
from jax.experimental import pallas as pl
from jax.experimental.pallas import tpu as pltpu
from jax.sharding import PartitionSpec as P

BF = jnp.bfloat16
F32 = jnp.float32
I32 = jnp.int32
NT = (((1,), (1,)), ((), ()))
AXES = ("gx", "gy", "gz")
LOGICAL = pl.DeviceIdType.LOGICAL
SIDES = ((1, 1, 0), (0, -1, 0), (3, 0, 1), (2, 0, -1), (1, 1, 1), (1, 1, -1), (0, -1, 1), (0, -1, -1))


def dotf(a, b):
    return jnp.dot(a, b, preferred_element_type=F32)


PB=32
UB=32
U=16
STEPS=((4,1),(2,2))
SB=8
TURN=tuple(27*u%128 for u in range(U))
STEP=27*SB%128

def row256(ref, j):
    r = ref[pl.ds(2*j,2),:]
    return jnp.concatenate([r[0:1],r[1:2]],axis=1)

def bucket(part, dest, ca, cb, out, cells, oh, pos_s, srt, csrt, acc, stv, sts, sem, peer, ship, ready, open_links):
    nb=32
    one=jnp.ones((),BF); zero=jnp.zeros((),BF)
    iod=lax.broadcasted_iota(I32,(128,256),0).astype(F32).astype(BF)
    def onehot(j,S):
        d=row256(dest,j).astype(F32).astype(BF)
        o=jnp.where(iod==jnp.broadcast_to(d,(128,256)),one,zero)
        oh[j]=o
        return S+o
    S=lax.fori_loop(0,nb,onehot,jnp.zeros((128,256),BF),unroll=4)
    ones=jnp.ones((256,256),BF)
    tot=dotf(S,ones)
    low=(lax.broadcasted_iota(I32,(128,128),0)>lax.broadcasted_iota(I32,(128,128),1)).astype(F32).astype(BF)
    start=dotf(low,tot.astype(BF))
    diag=lax.broadcasted_iota(I32,(128,128),0)==lax.broadcasted_iota(I32,(128,128),1)
    srow=jnp.sum(jnp.where(diag,start[:,:128],0.),axis=0,keepdims=True)
    trow=jnp.sum(jnp.where(diag,tot[:,:128],0.),axis=0,keepdims=True)
    tile=jnp.floor(srow*(1/128))
    sh=srow-128.*tile
    stv[0:1,:]=(tile+128.*(128.-sh)+32768.*trow).astype(I32)
    cp=pltpu.make_async_copy(stv,sts,sem)
    cp.start()
    up=(lax.broadcasted_iota(I32,(256,256),0)<lax.broadcasted_iota(I32,(256,256),1)).astype(F32).astype(BF)
    first=lax.broadcasted_iota(I32,(256,256),1)==0
    up=jnp.where(first,1.,up.astype(F32)).astype(BF)
    lane=lax.broadcasted_iota(I32,(128,256),1)
    def ranks(jj,base):
        for u in range(PB):
            j=jj*PB+u
            o=oh[j]
            x=dotf(o,up)
            b2=jnp.concatenate([base,base],axis=1)
            pos=jnp.sum(o.astype(F32)*(jnp.where(lane==0,0.,x)+b2),axis=0,keepdims=True)
            hi=jnp.floor(pos*(1/256))
            pos_s[j,0:1,:]=hi
            pos_s[j,1:2,:]=pos-256.*hi
            base=base+jnp.broadcast_to(x[:,0:1],(128,128))
        return base
    ranks(0,start[:,:128])
    ready()
    iol=lax.broadcasted_iota(I32,(256,256),0).astype(F32).astype(BF)
    s16=lax.broadcasted_iota(I32,(16,256),0)
    half=(s16//8).astype(F32).astype(BF)
    i32_=lax.broadcasted_iota(I32,(32,256),0).astype(F32).astype(BF)
    def place(jj,_):
        As=[];Ls=[]
        for u in range(UB):
            j=jj*UB+u
            hi=pos_s[j,0:1,:].astype(BF); lo=pos_s[j,1:2,:].astype(BF)
            lot=jnp.where(iol==jnp.broadcast_to(lo,(256,256)),one,zero)
            v=part[:,j*256:(j+1)*256]
            vh=v.astype(BF).astype(F32); vl=v-vh
            vh2=jnp.concatenate([vh,vh],axis=0).astype(BF)
            vl2=jnp.concatenate([vl,vl],axis=0).astype(BF)
            h16=jnp.broadcast_to(hi,(16,256))-half
            hs=[];ls=[]
            for k in range(16):
                m=h16==float(2*k)
                hs.append(jnp.where(m,vh2,zero)); ls.append(jnp.where(m,vl2,zero))
            m32=i32_==jnp.broadcast_to(hi,(32,256))
            a=row256(ca,j).astype(F32).astype(BF); b=row256(cb,j).astype(F32).astype(BF)
            As.append(jnp.concatenate(hs+ls+[jnp.where(m32,jnp.broadcast_to(a,(32,256)),zero),jnp.where(m32,jnp.broadcast_to(b,(32,256)),zero)],axis=0))
            Ls.append(lot)
        acc[...]=lax.dot_general(jnp.concatenate(As,axis=1),jnp.concatenate(Ls,axis=1),NT,preferred_element_type=F32)
        return _
    place(0,0)
    for h in range(32):
        x=acc[h*8:(h+1)*8]+acc[256+h*8:256+(h+1)*8]
        srt[2*h]=x[:,:128]; srt[2*h+1]=x[:,128:]
    cc=acc[512:544]*128.+acc[544:576]
    for t in range(64):
        r=cc[t//2:t//2+1,(t%2)*128:(t%2)*128+128]
        for i in range(3):
            if t-i>=0: csrt[t-i,i:i+1,:]=r
    cp.wait()
    lane=lax.broadcasted_iota(I32,(8,128),1)
    lane2=lane+128
    def expand(d):
        w=sts[0,d]
        t=w&127; rot=(w>>7)&255; n=w>>15
        rs=[pltpu.roll(srt[t+i],rot,1) for i in range(3)]
        c=pltpu.roll(csrt[t],rot,1)
        keep=lane<rot
        c1=jnp.where(keep[0:2],c[0:2],c[1:3])
        for i,at in enumerate((lane,lane2)):
            live=at<n
            out[d,:,128*i:128*(i+1)]=jnp.where(live,jnp.where(keep,rs[i],rs[i+1]),0.)
            cells[d,:,128*i:128*(i+1)]=jnp.where(live[0:1],c1[i:i+1],-1.)
    open_links()
    first=peer(0,0)
    second=wrap(first+STEP)
    for base in (first,second):
        for u in range(SB):
            expand(wrap(base+TURN[u]))
    ship(0,first,1)
    def deliver(m,base):
        now=wrap(base+STEP)
        for u in range(SB):
            expand(wrap(now+TURN[u]))
        ship((m-1)//(U//SB),base,0)
        return now
    last=lax.fori_loop(2,128//SB,deliver,second)
    ship(128//U-1,last,0)

def wrap(p):
    return jnp.where(p >= 128, p - 128, p)

def split(x):
    h=x.astype(BF); return h,(x-h.astype(F32)).astype(BF)
def weights(t):
    return 0.5*t*(t-1.), 1.-t*t, 0.5*t*(t+1.)
def setup(vel, halo, fh, fl, tab, masks):
    mu,md,ml,mr=masks
    lane=lax.broadcasted_iota(I32,(1,128),1)
    z8=jnp.zeros((8,256),F32)
    for c in range(2):
        ft=jnp.transpose(vel[c])
        lrow=halo[2][c:c+1,:]*ml
        rrow=halo[3][c:c+1,:]*mr
        e=jnp.concatenate([lrow,ft,rrow,jnp.zeros((6,256),F32)],axis=0)
        h,l=split(e)
        fh[c*136:(c+1)*136]=h; fl[c*136:(c+1)*136]=l
        rows=[]
        for (mid,lc,rc,m) in ((0,4,5,mu),(1,6,7,md)):
            r=halo[mid][c:c+1,:128]*m
            le=halo[lc][c:c+1,:128]*(m*ml); re=halo[rc][c:c+1,:128]*(m*mr)
            rows.append(jnp.where(lane==0,pltpu.roll(le,1,1),pltpu.roll(r,1,1)))
            rows.append(r)
            rows.append(jnp.where(lane==127,pltpu.roll(re,127,1),pltpu.roll(r,127,1)))
        tab[c]=jnp.concatenate(rows+[jnp.zeros((2,128),F32)],axis=0)
def cellparts(cell):
    cm=jnp.maximum(cell,0.)
    a=jnp.floor(cm*(1/128)); b=cm-128.*a
    return a,b
def pick(rows, bits):
    level=list(rows)
    for m in bits:
        level=[jnp.where(m,level[2*k+1],level[2*k]) for k in range(len(level)//2)]
    return level[0]
def interp(v, cell, fh, fl, tab):
    n=v.shape[1]
    zero=jnp.zeros((),BF)
    f=v[0:1]; g=v[1:2]
    live=cell>=0.
    a,b=cellparts(cell)
    wf=weights(f); wg=weights(g)
    ga=jnp.floor((a-1.)*(1/16)); oa=(a-1.)-16.*ga
    gab=jnp.broadcast_to(ga.astype(BF),(16,n))
    d=lax.broadcasted_iota(I32,(16,n),0).astype(F32).astype(BF)-jnp.broadcast_to(oa.astype(BF),(16,n))
    hl=[split(w) for w in wf]
    m0=d==0;m1=d==1;m2=d==2;q1=d==-15;q2=d==-14
    pats=[]
    for i in range(2):
        w=[jnp.broadcast_to(x[i],(16,n)) for x in hl]
        pats.append((jnp.where(m0,w[0],jnp.where(m1,w[1],jnp.where(m2,w[2],zero))),
                     jnp.where(q1,w[1],jnp.where(q2,w[2],zero))))
    ms=[gab==float(G) for G in range(-1,16)]
    W=[jnp.concatenate([jnp.where(ms[G+1],pa,jnp.where(ms[G],pb,zero)) for G in range(16)],axis=0) for pa,pb in pats]
    H=fh[...]; L=fl[...]
    R=dotf(H,W[0])+dotf(L,W[0])+dotf(H,W[1])
    gb=jnp.floor(b*(1/8)); ob=b-8.*gb
    s8=lax.broadcasted_iota(I32,(8,n),0).astype(F32)
    d8=s8-ob
    pa=jnp.where(d8==0,wg[0],jnp.where(d8==1,wg[1],jnp.where(d8==2,wg[2],0.)))
    pb=jnp.where(d8==-7,wg[1],jnp.where(d8==-6,wg[2],0.))
    gi=jnp.broadcast_to(gb,(8,n)).astype(I32)
    bits=[(gi&(1<<k))!=0 for k in range(4)]
    accs=[]
    for c in range(2):
        rows=[R[c*136+8*G:c*136+8*G+8] for G in range(17)]
        accs.append((pick(rows[:16],bits),pick(rows[1:],bits)))
    si=lax.broadcasted_iota(I32,(8,n),0)
    wj=jnp.where((si==0)|(si==3),wg[0],jnp.where((si==1)|(si==4),wg[1],wg[2]))
    up=jnp.where(a==0.,wf[0],0.); dn=jnp.where(a==255.,wf[2],0.)
    Pm=jnp.where(si<3,up,jnp.where(si<6,dn,0.))*wj
    bi=jnp.broadcast_to(b.astype(I32),(8,n))
    out=v
    for c in range(2):
        T=tab[c]
        corr=jnp.concatenate([jnp.take_along_axis(T,bi[:,128*i:128*(i+1)],axis=1) for i in range(n//128)],axis=1)
        sp=jnp.sum(pa*accs[c][0]+pb*accs[c][1]+Pm*corr,axis=0,keepdims=True)
        disp=jnp.where(live,0.5*sp,0.)
        out=out+jnp.where(si==2+c,disp,0.)
    return out


def fused(vel_in, part_in, dest_in, ca_in, cb_in, out, cout, vel, part, dest, ca, cb, send, scell, recv, rcell, edges, halo,
          fh, fl, tab, oh, pos_s, srt, csrt, acc, stv, sts, sem, ins, ss, ra, rb, rh):
    loads = [
        pltpu.make_async_copy(src, dst, ins.at[i])
        for i, (src, dst) in enumerate(((dest_in, dest), (vel_in, vel), (ca_in, ca), (cb_in, cb), (part_in, part)))
    ]
    for load in loads:
        load.start()
    gx = lax.axis_index("gx")
    col = lax.axis_index("gy") * 2 + lax.axis_index("gz")
    me = gx * 32 + col
    barrier = pltpu.get_barrier_semaphore()

    def other(k):
        return wrap(me + k)

    def peer(i, u):
        return wrap(other(lax.rem(i * (TURN[1] * U), 128)) + TURN[u])

    def origin(i, u):
        s = me - lax.rem(i * (TURN[1] * U), 128)
        s = jnp.where(s < 0, s + 128, s) - TURN[u]
        return jnp.where(s < 0, s + 128, s)

    for k in range(1, 128):
        pl.semaphore_signal(barrier, inc=1, device_id=other(k), device_id_type=LOGICAL)
    loads[0].wait()
    loads[1].wait()
    for c in range(2):
        zeros = jnp.zeros((1, 128), F32)
        edges[0, c : c + 1, :] = jnp.concatenate([vel[c, 0:1, :], zeros], axis=1)
        edges[1, c : c + 1, :] = jnp.concatenate([vel[c, 255:256, :], zeros], axis=1)
        turned = jnp.transpose(vel[c])
        edges[2, c : c + 1, :] = turned[0:1]
        edges[3, c : c + 1, :] = turned[127:128]

    def neighbour(da, db):
        return lax.rem(gx + da + 4, 4) * 32 + lax.rem(col + db + 32, 32)

    borders = []
    for slot, (edge, da, db) in enumerate(SIDES):
        borders.append(
            pltpu.make_async_remote_copy(
                src_ref=edges.at[edge],
                dst_ref=halo.at[slot],
                send_sem=ss.at[2],
                recv_sem=rh.at[slot],
                device_id=neighbour(da, db),
                device_id_type=LOGICAL,
            )
        )

    def ready():
        for load in loads[2:]:
            load.wait()

    def ship(group, base, at):
        for u in range(at, SB):
            p = wrap(base + TURN[u])
            for src, dst, lane_sem, done in ((send, recv, ss.at[0], ra), (scell, rcell, ss.at[1], rb)):
                pltpu.make_async_remote_copy(
                    src_ref=src.at[p],
                    dst_ref=dst.at[me],
                    send_sem=lane_sem,
                    recv_sem=done.at[group],
                    device_id=p,
                    device_id_type=LOGICAL,
                ).start()

    def open_links():
        pl.semaphore_wait(barrier, 127)
        for copy in borders:
            copy.start()

    bucket(part, dest, ca, cb, send, scell, oh, pos_s, srt, csrt, acc, stv, sts, sem, peer, ship, ready, open_links)
    recv[me] = send[me]
    rcell[me] = scell[me]

    def bytes_of(n, src, dst, s_sem, r_sem):
        return pltpu.make_async_remote_copy(
            src_ref=src.at[pl.ds(0, n)],
            dst_ref=dst.at[pl.ds(0, n)],
            send_sem=s_sem,
            recv_sem=r_sem,
            device_id=other(1),
            device_id_type=LOGICAL,
        )

    def arrived(group, n):
        bytes_of(n, send, recv, ss.at[0], ra.at[group]).wait_recv()
        bytes_of(n, scell, rcell, ss.at[1], rb.at[group]).wait_recv()

    for copy in borders:
        copy.wait_recv()
    masks = [(gx > 0).astype(F32), (gx < 3).astype(F32), (col > 0).astype(F32), (col < 31).astype(F32)]
    setup(vel, halo, fh, fl, tab, masks)
    def sources(group, count):
        for q in range(count):

            @pl.when(group + q > 0)
            def _full():
                arrived(group + q, U)

            if q == 0:

                @pl.when(group == 0)
                def _short():
                    arrived(0, U - 1)

        for q in range(count):
            for u in range(U):
                s = origin(group + q, u)
                cell = rcell[s]
                out[:, pl.ds(pl.multiple_of(s * 256, 256), 256)] = interp(recv[s], cell, fh, fl, tab)
                cout[s] = cell.astype(I32)

    done = 0
    for times, count in STEPS:

        def step(i, _, done=done, count=count):
            sources(done + i * count, count)
            return _

        lax.fori_loop(0, times, step, 0)
        done += times * count
    bytes_of(127, send, recv, ss.at[0], ra.at[0]).wait_send()
    bytes_of(127, scell, rcell, ss.at[1], rb.at[0]).wait_send()
    bytes_of(8, halo, halo, ss.at[2], rh.at[0]).wait_send()


def put_out(a_ref, b_ref, out, cout, sems):
    copies = [pltpu.make_async_copy(a_ref, out, sems.at[0]), pltpu.make_async_copy(b_ref, cout, sems.at[1])]
    for copy in copies:
        copy.start()
    for copy in copies:
        copy.wait()


def settle(binned, cells):
    binned, cells = pl.pallas_call(
        put_out,
        out_shape=(jax.ShapeDtypeStruct(binned.shape, F32), jax.ShapeDtypeStruct(cells.shape, I32)),
        in_specs=[pl.BlockSpec(memory_space=pltpu.VMEM)] * 2,
        out_specs=[pl.BlockSpec(memory_space=pl.ANY)] * 2,
        scratch_shapes=[pltpu.SemaphoreType.DMA((2,))],
        name="settle",
    )(pltpu.with_memory_space_constraint(binned, pltpu.VMEM), pltpu.with_memory_space_constraint(cells, pltpu.VMEM))
    return binned, cells.reshape(-1)


def shards(particles, dest_key, cell_a, cell_b, velocity):
    vmem = pl.BlockSpec(memory_space=pltpu.VMEM)
    binned, cells = pl.pallas_call(
        fused,
        out_shape=(pltpu.VMEM((8, 32768), F32), pltpu.VMEM((128, 1, 256), I32)),
        in_specs=[pl.BlockSpec(memory_space=pl.ANY)] * 5,
        out_specs=[vmem] * 2,
        scratch_shapes=[
            pltpu.VMEM((2, 256, 128), F32),
            pltpu.VMEM((8, 8192), F32),
            pltpu.VMEM((64, 128), I32),
            pltpu.VMEM((64, 128), I32),
            pltpu.VMEM((64, 128), I32),
            pltpu.VMEM((128, 8, 256), F32),
            pltpu.VMEM((128, 1, 256), F32),
            pltpu.VMEM((128, 8, 256), F32),
            pltpu.VMEM((128, 1, 256), F32),
            pltpu.VMEM((4, 2, 256), F32),
            pltpu.VMEM((8, 2, 256), F32),
            pltpu.VMEM((272, 256), BF),
            pltpu.VMEM((272, 256), BF),
            pltpu.VMEM((2, 8, 128), F32),
            pltpu.VMEM((32, 128, 256), BF),
            pltpu.VMEM((32, 2, 256), F32),
            pltpu.VMEM((130, 8, 128), F32),
            pltpu.VMEM((130, 8, 128), F32),
            pltpu.VMEM((576, 256), F32),
            pltpu.VMEM((8, 128), I32),
            pltpu.SMEM((8, 128), I32),
            pltpu.SemaphoreType.DMA,
            pltpu.SemaphoreType.DMA((5,)),
            pltpu.SemaphoreType.DMA((3,)),
            pltpu.SemaphoreType.DMA((128 // U,)),
            pltpu.SemaphoreType.DMA((128 // U,)),
            pltpu.SemaphoreType.DMA((8,)),
        ],
        compiler_params=pltpu.CompilerParams(collective_id=0, has_side_effects=True),
        name="rebin",
    )(velocity, particles, dest_key.reshape(64, 128), cell_a.reshape(64, 128), cell_b.reshape(64, 128))
    return settle(binned, cells)


def solution(mesh):
    in_specs = (P(None, AXES), P(AXES), P(AXES), P(AXES), P(None, "gx", ("gy", "gz")))
    return jax.shard_map(
        shards, mesh=mesh, in_specs=in_specs, out_specs=(P(None, AXES), P(AXES)), check_vma=False
    )
```
